32 devices in a mesh: gx: 4 (over x, core), gy: 2 (over y), gz: 4 (over z).
Axes of the slice: x: 2, y: 2, z: 4, core: 2. Of those that a mesh axis runs over, the one named last changes fastest.
Arguments:
- velocity: float32 [3, 512, 512], P(None, None, ('gx', 'gy', 'gz')), may hold values from -4 to 4
- inv_density: float32 [512, 512], P(None, ('gx', 'gy', 'gz')), may hold values from 0.25 to 4
- element_place: int32 [512], P(('gx', 'gy', 'gz')), may hold values from 0 to 15, as said below
Outputs:
- advected: float32 [3, 512, 512], P(None, None, ('gx', 'gy', 'gz'))
- pressure: float32 [512, 512], P(None, ('gx', 'gy', 'gz'))
- residual: float32 [512, 512], P(None, ('gx', 'gy', 'gz'))
The draws below stay inside these ranges and needn't reach their ends.
Inputs may be any that keep to these rules, and one draw needn't show every extreme that they name: `element_place`: within each device's 16 consecutive elements every block position appears exactly once.
All inputs are finite; a program needn't handle non-finite values.
Results may differ from the reference program's by a relative error of at most 0.0003.
Values sent between devices are 32-bit elements; how exact they have to be, the bound alone decides.
A program may use at most 64 MiB of HBM per device.

```python
import math
import jax
import jax.numpy as jnp
from jax import lax

PTS = 512
BX = 4
BY = 4
BZ = 1
CG_ITERS = 2
ELEM_DEV = 16
NEL = 512
N_GX = 4
N_GY = 2
N_GZ = 4


def shuffle_block(block_key):
    return jax.random.permutation(block_key, ELEM_DEV)


def draw_element_place(key, part):
    devices = NEL // ELEM_DEV
    device_keys = jax.random.split(jax.random.fold_in(key, 17), devices)
    orders = jax.vmap(shuffle_block)(device_keys)
    return orders.reshape(NEL).astype(jnp.int32)


def block_levels(key, dims, cuts, least, high):
    def one(dim, parts):
        steps = jax.random.uniform(jax.random.fold_in(jax.random.fold_in(key, 6), dim), (parts,), jnp.float32, least / len(cuts), high / len(cuts))
        return jnp.repeat(jnp.exp(steps), dims[dim] // parts).reshape((-1,) + (1,) * (len(dims) - dim - 1))

    factor_of = one(*cuts[0])
    for cut in cuts[1:]:
        factor_of = factor_of * one(*cut)
    return factor_of


def scatter_about(rng, extent, deviation, most, cuts=(), kind=jnp.bfloat16):
    level = block_levels(rng, extent, cuts, -0.22, 0.18) if cuts else 1.0
    values = jax.random.normal(rng, extent, jnp.float32) * deviation * level
    return jnp.minimum(jnp.maximum(values, -most), most).astype(kind)


def setup_inputs(seed: int = 0) -> dict:
    key_of = jax.random.split(jax.random.key(seed), 4)
    velocity = scatter_about(key_of[0], (3, PTS, NEL), 1.0, 4.0, ((2, 32),), jnp.float32)
    inv_density = jnp.clip(jnp.exp(math.log(4.0) - 2.7725887 * jax.random.uniform(key_of[1], (PTS, NEL), jnp.float32) ** block_levels(key_of[1], (PTS, NEL), ((1, 32),), -0.2, 0.2)), 0.25, 4.0)
    element_place = draw_element_place(jax.random.fold_in(key_of[3], 71), 0)
    return dict(velocity=velocity, inv_density=inv_density, element_place=element_place)


time_step = 0.03
mass_shift = 4.0
contractions = ("ij,sjbce->sibce", "ij,sajce->saice", "ij,sabje->sabie")
inner_nodes = (-0.8717401485096066, -0.5917001814331423, -0.2092992179024789, 0.2092992179024789, 0.5917001814331423, 0.8717401485096066)


def legendre_seven(position):
    previous = 1.0
    current_value = position
    for degree_index in range(1, 7):
        following = ((2 * degree_index + 1) * position * current_value - degree_index * previous) / (degree_index + 1)
        previous = current_value
        current_value = following
    return current_value


def tables():
    node_values = [-1.0] + list(inner_nodes) + [1.0]
    poly_values = [legendre_seven(node) for node in node_values]
    weights = [2.0 / (56.0 * value * value) for value in poly_values]
    derivative = [[0.0] * 8 for row_index in range(8)]
    for row_index in range(8):
        for col_index in range(8):
            if row_index != col_index:
                derivative[row_index][col_index] = poly_values[row_index] / (poly_values[col_index] * (node_values[row_index] - node_values[col_index]))
    derivative[0][0] = -14.0
    derivative[7][7] = 14.0
    squared_t = [[derivative[col_index][row_index] ** 2 for col_index in range(8)] for row_index in range(8)]
    quad_list = [weights[first] * weights[second] * weights[third] for first in range(8) for second in range(8) for third in range(8)]
    quadrature = jnp.asarray(quad_list, jnp.float32).reshape(1, 8, 8, 8, 1)
    return (quadrature, jnp.asarray(derivative, jnp.float32), jnp.asarray(squared_t, jnp.float32))


def apply_along(matrix, values, direction):
    return jnp.einsum(contractions[direction], matrix, values, precision=lax.Precision.HIGHEST)


def multiplicity(offsets, totals, block_shape, elements):
    slot_index = jnp.arange(elements, dtype=jnp.int32)
    places = (slot_index // (block_shape[1] * block_shape[2]), slot_index // block_shape[2] % block_shape[1], slot_index % block_shape[2])
    node_index = jnp.arange(8, dtype=jnp.int32)
    first_node = (node_index == 0).astype(jnp.float32)[:, None]
    last_node = (node_index == 7).astype(jnp.float32)[:, None]
    factors = []
    for direction in range(3):
        position = places[direction] + offsets[direction]
        lower_open = (position > 0).astype(jnp.float32)[None, :]
        upper_open = (position < totals[direction] - 1).astype(jnp.float32)[None, :]
        factors.append(1.0 + first_node * lower_open + last_node * upper_open)
    joined = factors[0][:, None, None, :] * factors[1][None, :, None, :] * factors[2][None, None, :, :]
    return joined[None]


def assemble_axis(values, point_axis, grid_axis, block_shape, sender):
    lower_faces = lax.index_in_dim(values, 0, point_axis, keepdims=False)
    upper_faces = lax.index_in_dim(values, 7, point_axis, keepdims=False)
    flat_shape = lower_faces.shape
    grid_shape = flat_shape[:3] + tuple(block_shape)
    lower_faces = lower_faces.reshape(grid_shape)
    upper_faces = upper_faces.reshape(grid_shape)
    element_axis = 3 + grid_axis
    length = block_shape[grid_axis]
    interior = lax.slice_in_dim(upper_faces, 0, length - 1, axis=element_axis) + lax.slice_in_dim(lower_faces, 1, length, axis=element_axis)
    lower_edge = lax.slice_in_dim(lower_faces, 0, 1, axis=element_axis)
    upper_edge = lax.slice_in_dim(upper_faces, length - 1, length, axis=element_axis)
    arrived = sender(jnp.stack([lower_edge, upper_edge]))
    first_sum = lower_edge + arrived[0]
    last_sum = upper_edge + arrived[3]
    new_lower = jnp.concatenate([first_sum, interior], axis=element_axis).reshape(flat_shape)
    new_upper = jnp.concatenate([interior, last_sum], axis=element_axis).reshape(flat_shape)
    values = lax.dynamic_update_slice_in_dim(values, jnp.expand_dims(new_lower, point_axis), 0, point_axis)
    values = lax.dynamic_update_slice_in_dim(values, jnp.expand_dims(new_upper, point_axis), 7, point_axis)
    return values


def pad_sender(face_pair):
    return jnp.pad(face_pair, [(1, 1)] + [(0, 0)] * (face_pair.ndim - 1))


def invert_order(ordering):
    return jnp.zeros((ordering.shape[0],), jnp.int32).at[ordering].set(jnp.arange(ordering.shape[0], dtype=jnp.int32))


def to_grid(array, inverse, devices):
    leading = array.shape[:-1]
    rank_lead = len(leading)
    blocks = array.reshape(leading + (devices, ELEM_DEV))
    index_full = jnp.broadcast_to(inverse.reshape((1,) * rank_lead + (devices, ELEM_DEV)), blocks.shape)
    blocks = jnp.take_along_axis(blocks, index_full, axis=-1)
    blocks = blocks.reshape(leading + (N_GX, N_GY, N_GZ, BX, BY, BZ))
    axes_order = list(range(rank_lead)) + [rank_lead + 0, rank_lead + 3, rank_lead + 1, rank_lead + 4, rank_lead + 2, rank_lead + 5]
    return blocks.transpose(axes_order).reshape(leading + (-1,))


def from_grid(array, orders, devices):
    leading = array.shape[:-1]
    rank_lead = len(leading)
    blocks = array.reshape(leading + (N_GX, BX, N_GY, BY, N_GZ, BZ))
    axes_order = list(range(rank_lead)) + [rank_lead + 0, rank_lead + 2, rank_lead + 4, rank_lead + 1, rank_lead + 3, rank_lead + 5]
    blocks = blocks.transpose(axes_order).reshape(leading + (devices, ELEM_DEV))
    index_full = jnp.broadcast_to(orders.reshape((1,) * rank_lead + (devices, ELEM_DEV)), blocks.shape)
    return jnp.take_along_axis(blocks, index_full, axis=-1).reshape(leading + (-1,))


def reference(velocity, inv_density, element_place):
    devices = N_GX * N_GY * N_GZ
    grid_shape = (BX * N_GX, BY * N_GY, BZ * N_GZ)
    orders = element_place.reshape(devices, ELEM_DEV)
    inverse = jax.vmap(invert_order)(orders)
    quadrature, derivative, square_table = tables()
    advector = to_grid(velocity, inverse, devices).reshape(3, 8, 8, 8, -1)
    mobility = to_grid(inv_density, inverse, devices).reshape(1, 8, 8, 8, -1)
    elements = advector.shape[-1]
    copies = multiplicity((0, 0, 0), grid_shape, grid_shape, elements)
    mass = quadrature * copies
    inverse_copies = 1.0 / copies

    def assemble(values):
        values = assemble_axis(values, 1, 0, grid_shape, pad_sender)
        values = assemble_axis(values, 2, 1, grid_shape, pad_sender)
        return assemble_axis(values, 3, 2, grid_shape, pad_sender)

    def advection_rate(section_value):
        convective = advector[0:1] * apply_along(derivative, section_value, 0)
        convective = convective + advector[1:2] * apply_along(derivative, section_value, 1)
        convective = convective + advector[2:3] * apply_along(derivative, section_value, 2)
        return assemble(-quadrature * convective) / mass

    first_rate = advection_rate(advector)
    second_rate = advection_rate(advector + 0.5 * time_step * first_rate)
    third_rate = advection_rate(advector + 0.5 * time_step * second_rate)
    fourth_rate = advection_rate(advector + time_step * third_rate)
    advected = advector + (time_step / 6.0) * (first_rate + 2.0 * second_rate + 2.0 * third_rate + fourth_rate)

    divergence = apply_along(derivative, advected[0:1], 0) + apply_along(derivative, advected[1:2], 1) + apply_along(derivative, advected[2:3], 2)
    weighted = quadrature * mobility
    diag_local = mass_shift * quadrature + apply_along(square_table, weighted, 0) + apply_along(square_table, weighted, 1) + apply_along(square_table, weighted, 2)
    source_local = -quadrature * divergence / time_step
    assembled = assemble(jnp.concatenate([source_local, diag_local], axis=0))
    source = assembled[0:1]
    inverse_jacobi = 1.0 / assembled[1:2]

    def operator(values):
        summed = mass_shift * quadrature * values
        for direction in range(3):
            slope = apply_along(derivative, values, direction)
            summed = summed + apply_along(derivative.T, weighted * slope, direction)
        return assemble(summed)

    def inner(left, right):
        return jnp.sum(left * right * inverse_copies)

    pressure = jnp.zeros_like(source)
    residual = source
    precond = residual * inverse_jacobi
    search = precond
    current = inner(residual, precond)
    for iteration in range(CG_ITERS):
        applied = operator(search)
        step_size = current / inner(search, applied)
        pressure = pressure + step_size * search
        residual = residual - step_size * applied
        if iteration + 1 < CG_ITERS:
            precond = residual * inverse_jacobi
            following = inner(residual, precond)
            search = precond + (following / current) * search
            current = following
    advected_out = from_grid(advected.reshape(3, 512, -1), orders, devices)
    pressure_out = from_grid(pressure.reshape(512, -1), orders, devices)
    residual_out = from_grid(residual.reshape(512, -1), orders, devices)
    return advected_out, pressure_out, residual_out
```

```python
import functools

import jax
import jax.numpy as jnp
import numpy as np
from jax import lax
from jax.experimental import pallas as pl
from jax.experimental.pallas import tpu as pltpu
from jax.sharding import PartitionSpec as P

BX = 4
BY = 4
BZ = 1
MESH = pl.DeviceIdType.MESH
AXES = ("gx", "gy", "gz")
ROUNDS = 7
VMEM_LIMIT = 16 << 20

time_step = 0.03
mass_shift = 4.0
inner_nodes = (
    -0.8717401485096066,
    -0.5917001814331423,
    -0.2092992179024789,
    0.2092992179024789,
    0.5917001814331423,
    0.8717401485096066,
)


def legendre_seven(position):
    previous = 1.0
    current_value = position
    for degree_index in range(1, 7):
        following = (
            (2 * degree_index + 1) * position * current_value - degree_index * previous
        ) / (degree_index + 1)
        previous = current_value
        current_value = following
    return current_value


def tables():
    nodes = [-1.0] + list(inner_nodes) + [1.0]
    poly = [legendre_seven(node) for node in nodes]
    weights = np.array([2.0 / (56.0 * value * value) for value in poly])
    derivative = np.zeros((8, 8))
    for i in range(8):
        for j in range(8):
            if i != j:
                derivative[i, j] = poly[i] / (poly[j] * (nodes[i] - nodes[j]))
    derivative[0, 0] = -14.0
    derivative[7, 7] = 14.0
    return weights, derivative.astype(np.float32).astype(np.float64)


def lane_rows(matrix):
    rows = np.zeros((32, 128))
    for t in range(4):
        for u in range(4):
            for h in range(2):
                rows[8 * t + 2 * u, 64 * h : 64 * h + 64] = matrix[2 * t + h, 2 * u + h]
                rows[8 * t + 2 * u + 1, 64 * h : 64 * h + 64] = matrix[2 * t + h, 2 * u + 1 - h]
    return rows


def split_stack(matrix):
    high = np.asarray(matrix, np.float32).astype(jnp.bfloat16)
    low = (np.asarray(matrix, np.float32) - high.astype(np.float32)).astype(jnp.bfloat16)
    return np.concatenate([high, high, low], axis=0)


@functools.cache
def constants():
    weights, d = tables()
    eye2, eye8, eye16 = np.eye(2), np.eye(8), np.eye(16)
    forward = np.concatenate(
        [np.kron(np.kron(eye2, d.T), eye8), np.kron(eye16, d.T)], axis=1
    )
    backward = np.concatenate([np.kron(np.kron(eye2, d), eye8), np.kron(eye16, d)], axis=0)
    square = np.kron(np.kron(eye2, d**2), eye8) + np.kron(eye16, d**2)
    quad = np.einsum("a,b,c->abc", weights, weights, weights).reshape(4, 128)
    rows = np.concatenate(
        [lane_rows(d), lane_rows(d.T), lane_rows(d.T**2), quad, np.zeros((4, 128))], axis=0
    )
    return (
        rows.astype(np.float32),
        split_stack(forward),
        split_stack(backward),
        split_stack(square),
    )


def kernel(
    counts,
    vel_ref,
    den_ref,
    place_ref,
    rows_ref,
    fwd_ref,
    bwd_ref,
    sqr_ref,
    adv_ref,
    pre_ref,
    res_ref,
    send_x,
    send_y,
    send_z,
    recv_xy,
    recv_z,
    sums,
    sums_in,
    send_sem,
    recv_sem,
    sum_send,
    sum_recv,
):
    f32 = jnp.float32
    me = [lax.axis_index(name) for name in AXES]
    has = [(me[i] > 0, me[i] < counts[i] - 1) for i in range(3)]

    def each_other(act):
        for kx in range(counts[0]):
            for ky in range(counts[1]):
                base = (kx * counts[1] + ky) * counts[2]
                first = 0 if base else 1

                def one(kz, _):
                    steps = (kx, ky, kz)
                    device = tuple(lax.rem(me[i] + steps[i], counts[i]) for i in range(3))
                    act(device, base + kz - 1)
                    return 0

                if counts[2] <= 8:
                    for kz in range(first, counts[2]):
                        one(kz, 0)
                else:
                    lax.fori_loop(first, counts[2], one, 0)

    directions = [
        (dx, dy, dz)
        for dx in (-1, 0, 1)
        for dy in (-1, 0, 1)
        for dz in (-1, 0, 1)
        if (dx, dy, dz) != (0, 0, 0)
    ]

    def exists(d):
        flag = None
        for i in range(3):
            if d[i]:
                here = has[i][1 if d[i] > 0 else 0]
                flag = here if flag is None else jnp.logical_and(flag, here)
        return flag

    def each_neighbour(act):
        for d in directions:

            @pl.when(exists(d))
            def _():
                act(tuple(me[i] + d[i] for i in range(3)), 0)

    barrier = pltpu.get_barrier_semaphore()

    def greet(device, index):
        pl.semaphore_signal(barrier, inc=1, device_id=device, device_id_type=MESH)

    if max(counts) <= ROUNDS:
        each_neighbour(greet)
        greeted = 1
        for i in range(3):
            low, high = has[i]
            greeted = greeted * (1 + low.astype(jnp.int32) + high.astype(jnp.int32))
        others = greeted - 1
    else:
        each_other(greet)
        others = counts[0] * counts[1] * counts[2] - 1

    lane = lax.broadcasted_iota(jnp.int32, (1, 16, 128), 2)
    row = lax.broadcasted_iota(jnp.int32, (1, 16, 128), 1)
    ex, ey = row // BY, row % BY
    node_b, node_c = (lane // 8) % 8, lane % 8

    r16 = lax.broadcasted_iota(jnp.int32, (16, 16), 0)
    l16 = lax.broadcasted_iota(jnp.int32, (16, 16), 1)
    by_lane = jnp.zeros((16, 16), jnp.int32)
    by_row = jnp.zeros((16, 16), jnp.int32)
    for e in range(16):
        by_lane = jnp.where(l16 == e, place_ref[e], by_lane)
        by_row = jnp.where(r16 == e, place_ref[e], by_row)
    to_place = (by_lane == r16).astype(f32)
    to_slot = (by_row == l16).astype(f32)

    def order(matrix, block):
        return jnp.dot(
            matrix, block, precision=lax.Precision.HIGHEST, preferred_element_type=f32
        )

    placed = [order(to_place, vel_ref[i]) for i in range(3)]
    velocity = [
        jnp.stack([placed[i][:, 128 * t : 128 * t + 128] for i in range(3)]) for t in range(4)
    ]
    dens = order(to_place, den_ref[...])
    quad = [rows_ref[96 + t : 97 + t, :].reshape(1, 1, 128) for t in range(4)]
    mobile = [quad[t] * dens[:, 128 * t : 128 * t + 128].reshape(1, 16, 128) for t in range(4)]

    def half(flag):
        return jnp.where(flag, 0.5, 1.0).astype(f32)

    total = [BX * counts[0], BY * counts[1], BZ * counts[2]]
    pos_x, pos_y = ex + me[0] * BX, ey + me[1] * BY
    share_y = half(
        ((node_b == 0) & (pos_y > 0)) | ((node_b == 7) & (pos_y < total[1] - 1))
    )
    pos_z = row * 0 + me[2]
    share_z = half(((node_c == 0) & (pos_z > 0)) | ((node_c == 7) & (pos_z < total[2] - 1)))
    share_yz = share_y * share_z
    share = [share_yz] * 4
    share[0] = share_yz * half((lane < 64) & (pos_x > 0))
    share[3] = share_yz * half((lane >= 64) & (pos_x < total[0] - 1))

    def along_x(base, v):
        swapped = [pltpu.roll(v[t], 64, 2) for t in range(4)]
        out = []
        for t in range(4):
            acc = None
            for u in range(4):
                k = base + 8 * t + 2 * u
                term = (
                    rows_ref[k : k + 1, :].reshape(1, 1, 128) * v[u]
                    + rows_ref[k + 1 : k + 2, :].reshape(1, 1, 128) * swapped[u]
                )
                acc = term if acc is None else acc + term
            out.append(acc)
        return out

    def split(x):
        high = x.astype(jnp.bfloat16)
        low = (x - high.astype(f32)).astype(jnp.bfloat16)
        return jnp.concatenate([high, low, high], axis=1)

    def along_lanes(v, w_ref):
        c = v[0].shape[0]
        x = jnp.concatenate([v[t].reshape(c * 16, -1) for t in range(4)], axis=0)
        y = jnp.dot(split(x), w_ref[...], preferred_element_type=f32)
        return [y[t * c * 16 : (t + 1) * c * 16].reshape(c, 16, -1) for t in range(4)]

    columns = [(dx, dy) for dx in (-1, 1, 0) for dy in (0, -1, 1)]
    cases = []
    if counts[2] > 2:
        cases.append(((-1, 0, 1), jnp.logical_and(has[2][0], has[2][1])))
    if counts[2] > 1:
        cases.append(((-1, 0), jnp.logical_not(has[2][1])))
        cases.append(((0, 1), jnp.logical_not(has[2][0])))
    else:
        cases.append(((0,), me[2] == 0))

    def code(d):
        return (d[0] + 1) * 9 + (d[1] + 1) * 3 + d[2] + 1

    def group(d):
        return (d[0] + 1) * 3 + d[1] + 1 if d[0] or d[1] else 9 + side_of(d[2])

    def side_of(step):
        return 1 if step > 0 else 0

    def source(r, d, c):
        if d[0]:
            return send_x.at[r, side_of(d[0])]
        if d[1]:
            return send_y.at[r, side_of(d[1])]
        return send_z.at[r, side_of(d[2]), pl.ds(0, c)]

    def target(r, d, c):
        if d[0] or d[1]:
            return recv_xy.at[r, code(d)]
        return recv_z.at[r, side_of(d[2]), pl.ds(0, c)]

    def copy(r, d, c, incoming):
        back = d if incoming else tuple(-i for i in d)
        return pltpu.make_async_remote_copy(
            src_ref=source(r, d, c),
            dst_ref=target(r, back, c),
            send_sem=send_sem.at[group(d)],
            recv_sem=recv_sem.at[r, group(back)],
            device_id=tuple(me[i] + d[i] for i in range(3)),
            device_id_type=MESH,
        )

    def each_column(act):
        for steps, flag in cases:

            @pl.when(flag)
            def _():
                for dx, dy in columns:
                    if dx or dy:

                        @pl.when(exists((dx, dy, 0)))
                        def _():
                            act(dx, dy, steps)

                    else:
                        act(dx, dy, [dz for dz in steps if dz])

    def start(r, c):
        def act(dx, dy, steps):
            for dz in steps:
                copy(r, (dx, dy, dz), c, False).start()

        each_column(act)

    def whole(ref, d, rounds_sem):
        return pltpu.make_async_remote_copy(
            src_ref=ref,
            dst_ref=ref,
            send_sem=send_sem.at[group(d)],
            recv_sem=rounds_sem.at[group(d)],
            device_id=tuple(me[i] + d[i] for i in range(3)),
            device_id_type=MESH,
        )

    def finish(r, c):
        def act(dx, dy, steps):
            if dx or dy:
                d = (dx, dy, 0)
                ref = recv_xy.at[r, pl.ds(code((dx, dy, steps[0])), len(steps))]
                whole(ref, d, recv_sem.at[r]).wait_recv()
            else:
                for dz in steps:
                    copy(r, (0, 0, dz), c, True).wait_recv()

        each_column(act)

    def sent():
        def act(dx, dy, steps):
            if dx or dy:
                d = (dx, dy, 0)
                ref = recv_xy.at[:, pl.ds(code((dx, dy, steps[0])), len(steps))]
                whole(ref, d, recv_sem.at[0]).wait_send()
            else:
                for dz in steps:
                    whole(recv_z.at[pl.ds(0, 2)], (0, 0, dz), recv_sem.at[0]).wait_send()

        each_column(act)

    for d in directions:

        @pl.when(jnp.logical_not(exists(d)))
        def _():
            for r in range(ROUNDS):
                if d[0] or d[1]:
                    recv_xy[r, code(d)] = jnp.zeros((8, 128), f32)
                else:
                    recv_z[r, side_of(d[2])] = jnp.zeros((4, 8, 128), f32)

    sub8 = lax.broadcasted_iota(jnp.int32, (8, 128), 0)
    lane8 = lax.broadcasted_iota(jnp.int32, (8, 128), 1)
    quarter = sub8 // 4 + 2 * (lane8 // 64)
    b8, c8, y8 = (lane8 // 8) % 8, lane8 % 8, sub8 % 4

    def turn(x, shift, axis):
        size = x.shape[axis]
        shift = shift % size
        return pltpu.roll(x, shift, axis) if shift else x

    def requarter(x, k, base):
        if (k ^ base) & 1:
            x = turn(x, 4, 0)
        if (k ^ base) & 2:
            x = turn(x, 64, 1)
        return x

    def z_joined(r, dx, dy):
        mid = recv_xy[r, code((dx, dy, 0))]
        low = turn(recv_xy[r, code((dx, dy, -1))], -7, 1)
        high = turn(recv_xy[r, code((dx, dy, 1))], 7, 1)
        return mid + jnp.where(c8 == 0, low, jnp.where(c8 == 7, high, 0.0))

    def assemble(v, r, hook=None):
        v = list(v)
        c = v[0].shape[0]
        lower, upper = turn(v[0], 64, 2), turn(v[3], 64, 2)
        v[0] = v[0] + jnp.where((lane < 64) & (row >= 4), turn(upper, 4, 1), 0.0)
        v[3] = v[3] + jnp.where((lane >= 64) & (row < 12), turn(lower, -4, 1), 0.0)
        lower = v[0]
        upper = turn(v[0], 72, 2)
        for t in range(1, 4):
            lower = jnp.where(node_b == t, turn(v[t], 8 * t, 2), lower)
            upper = jnp.where(node_b == t, turn(v[t], 72 + 8 * t, 2), upper)
        d_low = jnp.where(ey > 0, turn(upper, 1, 1), 0.0)
        d_high = jnp.where(ey < 3, turn(lower, -1, 1), 0.0)

        def add_y(d_low, d_high):
            for t in range(4):
                low, high = turn(d_low, -8 * t, 2), turn(d_high, 56 - 8 * t, 2)
                v[t] = v[t] + jnp.where(node_b == 0, low, jnp.where(node_b == 7, high, 0.0))

        add_y(d_low, d_high)
        lower, upper = lower + d_low, upper + d_high
        for side in range(2):
            base = 3 * side
            acc = None
            for k in range(c):
                part = requarter(v[3 * side][k, 8 * side : 8 * side + 8], k, base)
                acc = part if acc is None else jnp.where(quarter == k, part, acc)
            send_x[r, side] = acc
        for side, face in ((0, lower), (1, upper)):
            acc = None
            for k in range(c):
                part = jnp.where(b8 < 4, face[k, 0:8], turn(face[k, 8:16], 32, 1))
                part = turn(part, k + 5 * side, 0)
                acc = part if acc is None else jnp.where(y8 == k, part, acc)
            send_y[r, side] = acc
        lower = v[0]
        upper = turn(v[0], -7, 2)
        for t in range(1, 4):
            lower = jnp.where(node_c == t, turn(v[t], t, 2), lower)
            upper = jnp.where(node_c == t, turn(v[t], t - 7, 2), upper)
        for side, face in ((0, lower), (1, upper)):
            for k in range(c):
                send_z[r, side, k] = jnp.where(c8 < 4, face[k, 0:8], turn(face[k, 8:16], 4, 1))
        start(r, c)
        if hook is not None:
            hook()
        finish(r, c)
        for side in range(2):
            dx = 2 * side - 1
            low = turn(turn(z_joined(r, dx, -1), -56, 1), -3, 0)
            high = turn(turn(z_joined(r, dx, 1), 56, 1), 3, 0)
            face = z_joined(r, dx, 0) + jnp.where(
                (y8 == 0) & (b8 == 0), low, jnp.where((y8 == 3) & (b8 == 7), high, 0.0)
            )
            base = 3 * side
            parts = [
                jnp.where(quarter == base, requarter(face, k, base), 0.0) for k in range(c)
            ]
            part = jnp.stack(parts)
            zero = jnp.zeros_like(part)
            pair = [part, zero] if side == 0 else [zero, part]
            v[3 * side] = v[3 * side] + jnp.concatenate(pair, axis=1)
        got = []
        for side in range(2):
            face = z_joined(r, 0, 2 * side - 1)
            parts = []
            for k in range(c):
                part = jnp.where(y8 == 3 * side, turn(face, 3 * side - k, 0), 0.0)
                parts.append(jnp.concatenate([part, turn(part, -32, 1)], axis=0))
            got.append(jnp.stack(parts))
        add_y(got[0], got[1])
        got = []
        for side in range(2):
            face = recv_z[r, side, :c]
            got.append(jnp.concatenate([face, turn(face, -4, 2)], axis=1))
        for t in range(4):
            low, high = turn(got[0], -t, 2), turn(got[1], 7 - t, 2)
            v[t] = v[t] + jnp.where(node_c == 0, low, jnp.where(node_c == 7, high, 0.0))
        return v

    def advect(v):
        dx = along_x(0, v)
        dyz = along_lanes(v, fwd_ref)
        return [
            velocity[t][0:1] * dx[t]
            + velocity[t][1:2] * dyz[t][:, :, :128]
            + velocity[t][2:3] * dyz[t][:, :, 128:]
            for t in range(4)
        ]

    first = advect(velocity)
    diag = []

    def diagonal():
        square_x = along_x(64, mobile)
        square_yz = along_lanes(mobile, sqr_ref)
        diag.extend(mass_shift * quad[t] + square_x[t] + square_yz[t] for t in range(4))

    pl.semaphore_wait(barrier, others)
    first = assemble(first, 0, diagonal)
    k1 = [first[t] * share[t] for t in range(4)]
    total_rate = k1
    v = [velocity[t] - (0.5 * time_step) * k1[t] for t in range(4)]
    for r, step, weight in ((1, 0.5, 2.0), (2, 1.0, 2.0), (3, 0.0, 1.0)):
        g = advect(v)
        if r == 1:
            g = assemble([jnp.concatenate([g[t], diag[t]], axis=0) for t in range(4)], r)
            inverse_jacobi = [1.0 / g[t][3:4] for t in range(4)]
            g = [g[t][0:3] for t in range(4)]
        else:
            g = assemble(g, r)
        g = [g[t] * share[t] for t in range(4)]
        total_rate = [total_rate[t] + weight * g[t] for t in range(4)]
        if step:
            v = [velocity[t] - (step * time_step) * g[t] for t in range(4)]
    advected = [velocity[t] - (time_step / 6.0) * total_rate[t] for t in range(4)]

    dx = along_x(0, [advected[t][0:1] for t in range(4)])
    dyz = along_lanes([advected[t][1:3] for t in range(4)], fwd_ref)
    div = [dx[t] + dyz[t][0:1, :, :128] + dyz[t][1:2, :, 128:] for t in range(4)]
    def put(field):
        return order(to_slot, field)

    def put_advected():
        for i in range(3):
            adv_ref[i] = put(jnp.concatenate([advected[t][i] for t in range(4)], axis=1))

    total_div = assemble(div, 4, put_advected)
    r0 = [total_div[t] * (quad[t] * (-1.0 / time_step)) for t in range(4)]

    def local(v):
        dx = along_x(0, v)
        dyz = along_lanes(v, fwd_ref)
        gx = [mobile[t] * dx[t] for t in range(4)]
        gyz = [
            jnp.concatenate(
                [mobile[t] * dyz[t][:, :, :128], mobile[t] * dyz[t][:, :, 128:]], axis=2
            )
            for t in range(4)
        ]
        bx = along_x(32, gx)
        byz = along_lanes(gyz, bwd_ref)
        return [(mass_shift * quad[t]) * v[t] + bx[t] + byz[t] for t in range(4)]

    def dot_row(a, b, scale=None):
        acc = None
        for t in range(4):
            term = a[t] * b[t]
            if scale is not None:
                term = term * scale[t]
            acc = term if acc is None else acc + term
        return jnp.sum(acc[0], axis=0, keepdims=True)

    z0 = [r0[t] * inverse_jacobi[t] for t in range(4)]
    lz = local(z0)
    rho_row = dot_row(r0, z0, share)
    gamma_row = dot_row(z0, lz)
    s = assemble(lz, 5)
    w = [s[t] * inverse_jacobi[t] for t in range(4)]
    lw = local(w)
    delta_row = dot_row(s, w, share)
    eps_row = dot_row(w, lw)
    partial = jnp.concatenate(
        [rho_row, gamma_row, delta_row, eps_row, jnp.zeros((4, 128), f32)], axis=0
    )
    partial = jnp.sum(partial, axis=1, keepdims=True)
    own = jnp.sum(jnp.where(sub8 == lane8, partial, 0.0), axis=0, keepdims=True)
    sums[...] = own

    def share_sums(device, index):
        pltpu.make_async_remote_copy(
            src_ref=sums,
            dst_ref=sums_in.at[index],
            send_sem=sum_send,
            recv_sem=sum_recv,
            device_id=device,
            device_id_type=MESH,
        ).start()

    each_other(share_sums)
    t_vec = assemble(lw, 6)
    arrived = pltpu.make_async_remote_copy(
        src_ref=sums_in,
        dst_ref=sums_in,
        send_sem=sum_send,
        recv_sem=sum_recv,
        device_id=tuple(lax.rem(me[i] + 1, counts[i]) for i in range(3)),
        device_id_type=MESH,
    )
    arrived.wait_recv()
    joined = own + jnp.sum(sums_in[...], axis=0)
    four = jnp.sum(jnp.where(sub8 == lane8, joined, 0.0), axis=1, keepdims=True)
    rho, gamma, delta, eps = (four[i : i + 1].reshape(1, 1, 1) for i in range(4))
    alpha0 = rho / gamma
    rho1 = rho - 2.0 * alpha0 * gamma + alpha0 * alpha0 * delta
    beta = rho1 / rho
    cross = gamma - alpha0 * delta
    curve = gamma - 2.0 * alpha0 * delta + alpha0 * alpha0 * eps
    curve = curve + 2.0 * beta * cross + beta * beta * gamma
    alpha1 = rho1 / curve
    along = alpha0 + alpha1 * (1.0 + beta)
    side_step = alpha0 * alpha1

    pre_ref[...] = put(
        jnp.concatenate([(along * z0[t] - side_step * w[t])[0] for t in range(4)], axis=1)
    )
    res_ref[...] = put(
        jnp.concatenate(
            [(r0[t] - along * s[t] + side_step * t_vec[t])[0] for t in range(4)], axis=1
        )
    )
    sent()
    arrived.wait_send()


def finish_kernel(adv_ref, pre_ref, res_ref, adv_out, pre_out, res_out):
    adv_out[...] = adv_ref[...]
    pre_out[...] = pre_ref[...]
    res_out[...] = res_ref[...]


def per_device(counts, velocity, inv_density, element_place):
    f32 = jnp.float32
    rows, forward, backward, square = constants()
    elements = element_place.shape[0]
    points = inv_density.shape[0]
    vmem = pl.BlockSpec(memory_space=pltpu.VMEM)
    faces = pltpu.VMEM((ROUNDS, 2, 8, 128), f32)
    faces_z = pltpu.VMEM((ROUNDS, 2, 4, 8, 128), f32)
    dma = pltpu.SemaphoreType.DMA
    others = counts[0] * counts[1] * counts[2] - 1
    shapes = (
        jax.ShapeDtypeStruct((3, elements, points), f32),
        jax.ShapeDtypeStruct((elements, points), f32),
        jax.ShapeDtypeStruct((elements, points), f32),
    )
    computed = pl.pallas_call(
        functools.partial(kernel, counts),
        out_shape=shapes,
        in_specs=[vmem, vmem, pl.BlockSpec(memory_space=pltpu.SMEM), vmem, vmem, vmem, vmem],
        out_specs=(vmem, vmem, vmem),
        scratch_shapes=[
            faces,
            faces,
            faces_z,
            pltpu.VMEM((ROUNDS, 27, 8, 128), f32),
            faces_z,
            pltpu.VMEM((1, 128), f32),
            pltpu.VMEM((others, 1, 128), f32),
            dma((11,)),
            dma((ROUNDS, 11)),
            dma,
            dma,
        ],
        compiler_params=pltpu.CompilerParams(
            collective_id=0, has_side_effects=True, vmem_limit_bytes=VMEM_LIMIT
        ),
    )(
        velocity.transpose(0, 2, 1),
        inv_density.T,
        element_place,
        jnp.asarray(rows),
        jnp.asarray(forward),
        jnp.asarray(backward),
        jnp.asarray(square),
    )
    advected, pressure, residual = pl.pallas_call(
        finish_kernel,
        out_shape=shapes,
        in_specs=[vmem, vmem, vmem],
        out_specs=(vmem, vmem, vmem),
        compiler_params=pltpu.CompilerParams(vmem_limit_bytes=VMEM_LIMIT),
    )(*computed)
    return advected.transpose(0, 2, 1), pressure.T, residual.T


def solution(mesh):
    counts = tuple(mesh.shape[name] for name in AXES)
    placed = (P(None, None, AXES), P(None, AXES), P(AXES))
    return jax.shard_map(
        functools.partial(per_device, counts),
        mesh=mesh,
        in_specs=placed,
        out_specs=(P(None, None, AXES), P(None, AXES), P(None, AXES)),
        check_vma=False,
    )
```

```python
import functools

import jax
import jax.numpy as jnp
import numpy as np
from jax import lax
from jax.experimental import pallas as pl
from jax.experimental.pallas import tpu as pltpu
from jax.sharding import PartitionSpec as P

BX = 4
BY = 4
BZ = 1
MESH = pl.DeviceIdType.MESH
AXES = ("gx", "gy", "gz")
ROUNDS = 7
VMEM_LIMIT = 16 << 20

time_step = 0.03
mass_shift = 4.0
inner_nodes = (
    -0.8717401485096066,
    -0.5917001814331423,
    -0.2092992179024789,
    0.2092992179024789,
    0.5917001814331423,
    0.8717401485096066,
)


def legendre_seven(position):
    previous = 1.0
    current_value = position
    for degree_index in range(1, 7):
        following = (
            (2 * degree_index + 1) * position * current_value - degree_index * previous
        ) / (degree_index + 1)
        previous = current_value
        current_value = following
    return current_value


def tables():
    nodes = [-1.0] + list(inner_nodes) + [1.0]
    poly = [legendre_seven(node) for node in nodes]
    weights = np.array([2.0 / (56.0 * value * value) for value in poly])
    derivative = np.zeros((8, 8))
    for i in range(8):
        for j in range(8):
            if i != j:
                derivative[i, j] = poly[i] / (poly[j] * (nodes[i] - nodes[j]))
    derivative[0, 0] = -14.0
    derivative[7, 7] = 14.0
    return weights, derivative.astype(np.float32).astype(np.float64)


def lane_rows(matrix):
    rows = np.zeros((32, 128))
    for t in range(4):
        for u in range(4):
            for h in range(2):
                rows[8 * t + 2 * u, 64 * h : 64 * h + 64] = matrix[2 * t + h, 2 * u + h]
                rows[8 * t + 2 * u + 1, 64 * h : 64 * h + 64] = matrix[2 * t + h, 2 * u + 1 - h]
    return rows


def split_stack(matrix):
    high = np.asarray(matrix, np.float32).astype(jnp.bfloat16)
    low = (np.asarray(matrix, np.float32) - high.astype(np.float32)).astype(jnp.bfloat16)
    return np.concatenate([high, high, low], axis=0)


@functools.cache
def constants():
    weights, d = tables()
    eye2, eye8, eye16 = np.eye(2), np.eye(8), np.eye(16)
    forward = np.concatenate(
        [np.kron(np.kron(eye2, d.T), eye8), np.kron(eye16, d.T)], axis=1
    )
    backward = np.concatenate([np.kron(np.kron(eye2, d), eye8), np.kron(eye16, d)], axis=0)
    square = np.kron(np.kron(eye2, d**2), eye8) + np.kron(eye16, d**2)
    quad = np.einsum("a,b,c->abc", weights, weights, weights).reshape(4, 128)
    rows = np.concatenate(
        [lane_rows(d), lane_rows(d.T), lane_rows(d.T**2), quad, np.zeros((4, 128))], axis=0
    )
    return (
        rows.astype(np.float32),
        split_stack(forward),
        split_stack(backward),
        split_stack(square),
    )


def kernel(
    counts,
    vel_hbm,
    den_hbm,
    place_hbm,
    rows_hbm,
    fwd_hbm,
    bwd_hbm,
    sqr_hbm,
    adv_ref,
    pre_ref,
    res_ref,
    send_x,
    send_y,
    send_z,
    recv_xy,
    recv_z,
    sums,
    sums_in,
    send_sem,
    recv_sem,
    sum_send,
    sum_recv,
    vel_ref,
    den_ref,
    place_ref,
    rows_ref,
    fwd_ref,
    bwd_ref,
    sqr_ref,
    load_sem,
):
    f32 = jnp.float32
    loads = [
        pltpu.make_async_copy(source_ref, target_ref, load_sem.at[index])
        for index, (source_ref, target_ref) in enumerate(
            (
                (place_hbm, place_ref),
                (vel_hbm, vel_ref),
                (rows_hbm, rows_ref),
                (fwd_hbm, fwd_ref),
                (den_hbm, den_ref),
                (sqr_hbm, sqr_ref),
                (bwd_hbm, bwd_ref),
            )
        )
    ]
    for load in loads:
        load.start()
    me = [lax.axis_index(name) for name in AXES]
    has = [(me[i] > 0, me[i] < counts[i] - 1) for i in range(3)]

    def each_other(act):
        for kx in range(counts[0]):
            for ky in range(counts[1]):
                base = (kx * counts[1] + ky) * counts[2]
                first = 0 if base else 1

                def one(kz, _):
                    steps = (kx, ky, kz)
                    device = tuple(lax.rem(me[i] + steps[i], counts[i]) for i in range(3))
                    act(device, base + kz - 1)
                    return 0

                if counts[2] <= 8:
                    for kz in range(first, counts[2]):
                        one(kz, 0)
                else:
                    lax.fori_loop(first, counts[2], one, 0)

    directions = [
        (dx, dy, dz)
        for dx in (-1, 0, 1)
        for dy in (-1, 0, 1)
        for dz in (-1, 0, 1)
        if (dx, dy, dz) != (0, 0, 0)
    ]

    def exists(d):
        flag = None
        for i in range(3):
            if d[i]:
                here = has[i][1 if d[i] > 0 else 0]
                flag = here if flag is None else jnp.logical_and(flag, here)
        return flag

    def each_neighbour(act):
        for d in directions:

            @pl.when(exists(d))
            def _():
                act(tuple(me[i] + d[i] for i in range(3)), 0)

    barrier = pltpu.get_barrier_semaphore()

    def greet(device, index):
        pl.semaphore_signal(barrier, inc=1, device_id=device, device_id_type=MESH)

    if max(counts) <= ROUNDS:
        each_neighbour(greet)
        greeted = 1
        for i in range(3):
            low, high = has[i]
            greeted = greeted * (1 + low.astype(jnp.int32) + high.astype(jnp.int32))
        others = greeted - 1
    else:
        each_other(greet)
        others = counts[0] * counts[1] * counts[2] - 1

    lane = lax.broadcasted_iota(jnp.int32, (1, 16, 128), 2)
    row = lax.broadcasted_iota(jnp.int32, (1, 16, 128), 1)
    ex, ey = row // BY, row % BY
    node_b, node_c = (lane // 8) % 8, lane % 8

    loads[0].wait()
    r16 = lax.broadcasted_iota(jnp.int32, (16, 16), 0)
    l16 = lax.broadcasted_iota(jnp.int32, (16, 16), 1)
    by_lane = jnp.zeros((16, 16), jnp.int32)
    by_row = jnp.zeros((16, 16), jnp.int32)
    for e in range(16):
        by_lane = jnp.where(l16 == e, place_ref[e], by_lane)
        by_row = jnp.where(r16 == e, place_ref[e], by_row)
    to_place = (by_lane == r16).astype(f32)
    to_slot = (by_row == l16).astype(f32)

    def order(matrix, block):
        return jnp.dot(
            matrix, block, precision=lax.Precision.HIGHEST, preferred_element_type=f32
        )

    loads[1].wait()
    placed = [order(to_place, vel_ref[i]) for i in range(3)]
    velocity = [
        jnp.stack([placed[i][:, 128 * t : 128 * t + 128] for i in range(3)]) for t in range(4)
    ]
    loads[2].wait()
    quad = [rows_ref[96 + t : 97 + t, :].reshape(1, 1, 128) for t in range(4)]

    def half(flag):
        return jnp.where(flag, 0.5, 1.0).astype(f32)

    total = [BX * counts[0], BY * counts[1], BZ * counts[2]]
    pos_x, pos_y = ex + me[0] * BX, ey + me[1] * BY
    share_y = half(
        ((node_b == 0) & (pos_y > 0)) | ((node_b == 7) & (pos_y < total[1] - 1))
    )
    pos_z = row * 0 + me[2]
    share_z = half(((node_c == 0) & (pos_z > 0)) | ((node_c == 7) & (pos_z < total[2] - 1)))
    share_yz = share_y * share_z
    share = [share_yz] * 4
    share[0] = share_yz * half((lane < 64) & (pos_x > 0))
    share[3] = share_yz * half((lane >= 64) & (pos_x < total[0] - 1))

    def along_x(base, v):
        swapped = [pltpu.roll(v[t], 64, 2) for t in range(4)]
        out = []
        for t in range(4):
            acc = None
            for u in range(4):
                k = base + 8 * t + 2 * u
                term = (
                    rows_ref[k : k + 1, :].reshape(1, 1, 128) * v[u]
                    + rows_ref[k + 1 : k + 2, :].reshape(1, 1, 128) * swapped[u]
                )
                acc = term if acc is None else acc + term
            out.append(acc)
        return out

    def split(x):
        high = x.astype(jnp.bfloat16)
        low = (x - high.astype(f32)).astype(jnp.bfloat16)
        return jnp.concatenate([high, low, high], axis=1)

    def along_lanes(v, w_ref):
        c = v[0].shape[0]
        x = jnp.concatenate([v[t].reshape(c * 16, -1) for t in range(4)], axis=0)
        y = jnp.dot(split(x), w_ref[...], preferred_element_type=f32)
        return [y[t * c * 16 : (t + 1) * c * 16].reshape(c, 16, -1) for t in range(4)]

    columns = [(dx, dy) for dx in (-1, 1, 0) for dy in (0, -1, 1)]
    cases = []
    if counts[2] > 2:
        cases.append(((-1, 0, 1), jnp.logical_and(has[2][0], has[2][1])))
    if counts[2] > 1:
        cases.append(((-1, 0), jnp.logical_not(has[2][1])))
        cases.append(((0, 1), jnp.logical_not(has[2][0])))
    else:
        cases.append(((0,), me[2] == 0))

    def code(d):
        return (d[0] + 1) * 9 + (d[1] + 1) * 3 + d[2] + 1

    def group(d):
        return (d[0] + 1) * 3 + d[1] + 1 if d[0] or d[1] else 9 + side_of(d[2])

    def side_of(step):
        return 1 if step > 0 else 0

    def source(r, d, c):
        if d[0]:
            return send_x.at[r, side_of(d[0])]
        if d[1]:
            return send_y.at[r, side_of(d[1])]
        return send_z.at[r, side_of(d[2]), pl.ds(0, c)]

    def target(r, d, c):
        if d[0] or d[1]:
            return recv_xy.at[r, code(d)]
        return recv_z.at[r, side_of(d[2]), pl.ds(0, c)]

    def copy(r, d, c, incoming):
        back = d if incoming else tuple(-i for i in d)
        return pltpu.make_async_remote_copy(
            src_ref=source(r, d, c),
            dst_ref=target(r, back, c),
            send_sem=send_sem.at[group(d)],
            recv_sem=recv_sem.at[r, group(back)],
            device_id=tuple(me[i] + d[i] for i in range(3)),
            device_id_type=MESH,
        )

    def each_column(act):
        for steps, flag in cases:

            @pl.when(flag)
            def _():
                for dx, dy in columns:
                    if dx or dy:

                        @pl.when(exists((dx, dy, 0)))
                        def _():
                            act(dx, dy, steps)

                    else:
                        act(dx, dy, [dz for dz in steps if dz])

    def start(r, c):
        def act(dx, dy, steps):
            for dz in steps:
                copy(r, (dx, dy, dz), c, False).start()

        each_column(act)

    def whole(ref, d, rounds_sem):
        return pltpu.make_async_remote_copy(
            src_ref=ref,
            dst_ref=ref,
            send_sem=send_sem.at[group(d)],
            recv_sem=rounds_sem.at[group(d)],
            device_id=tuple(me[i] + d[i] for i in range(3)),
            device_id_type=MESH,
        )

    def finish(r, c):
        def act(dx, dy, steps):
            if dx or dy:
                d = (dx, dy, 0)
                ref = recv_xy.at[r, pl.ds(code((dx, dy, steps[0])), len(steps))]
                whole(ref, d, recv_sem.at[r]).wait_recv()
            else:
                for dz in steps:
                    copy(r, (0, 0, dz), c, True).wait_recv()

        each_column(act)

    def sent():
        def act(dx, dy, steps):
            if dx or dy:
                d = (dx, dy, 0)
                ref = recv_xy.at[:, pl.ds(code((dx, dy, steps[0])), len(steps))]
                whole(ref, d, recv_sem.at[0]).wait_send()
            else:
                for dz in steps:
                    whole(recv_z.at[pl.ds(0, 2)], (0, 0, dz), recv_sem.at[0]).wait_send()

        each_column(act)

    for d in directions:

        @pl.when(jnp.logical_not(exists(d)))
        def _():
            for r in range(ROUNDS):
                if d[0] or d[1]:
                    recv_xy[r, code(d)] = jnp.zeros((8, 128), f32)
                else:
                    recv_z[r, side_of(d[2])] = jnp.zeros((4, 8, 128), f32)

    sub8 = lax.broadcasted_iota(jnp.int32, (8, 128), 0)
    lane8 = lax.broadcasted_iota(jnp.int32, (8, 128), 1)
    quarter = sub8 // 4 + 2 * (lane8 // 64)
    b8, c8, y8 = (lane8 // 8) % 8, lane8 % 8, sub8 % 4

    def turn(x, shift, axis):
        size = x.shape[axis]
        shift = shift % size
        return pltpu.roll(x, shift, axis) if shift else x

    def requarter(x, k, base):
        if (k ^ base) & 1:
            x = turn(x, 4, 0)
        if (k ^ base) & 2:
            x = turn(x, 64, 1)
        return x

    def z_joined(r, dx, dy):
        mid = recv_xy[r, code((dx, dy, 0))]
        low = turn(recv_xy[r, code((dx, dy, -1))], -7, 1)
        high = turn(recv_xy[r, code((dx, dy, 1))], 7, 1)
        return mid + jnp.where(c8 == 0, low, jnp.where(c8 == 7, high, 0.0))

    def assemble(v, r, hook=None):
        v = list(v)
        c = v[0].shape[0]
        lower, upper = turn(v[0], 64, 2), turn(v[3], 64, 2)
        v[0] = v[0] + jnp.where((lane < 64) & (row >= 4), turn(upper, 4, 1), 0.0)
        v[3] = v[3] + jnp.where((lane >= 64) & (row < 12), turn(lower, -4, 1), 0.0)
        lower = v[0]
        upper = turn(v[0], 72, 2)
        for t in range(1, 4):
            lower = jnp.where(node_b == t, turn(v[t], 8 * t, 2), lower)
            upper = jnp.where(node_b == t, turn(v[t], 72 + 8 * t, 2), upper)
        d_low = jnp.where(ey > 0, turn(upper, 1, 1), 0.0)
        d_high = jnp.where(ey < 3, turn(lower, -1, 1), 0.0)

        def add_y(d_low, d_high):
            for t in range(4):
                low, high = turn(d_low, -8 * t, 2), turn(d_high, 56 - 8 * t, 2)
                v[t] = v[t] + jnp.where(node_b == 0, low, jnp.where(node_b == 7, high, 0.0))

        add_y(d_low, d_high)
        lower, upper = lower + d_low, upper + d_high
        for side in range(2):
            base = 3 * side
            acc = None
            for k in range(c):
                part = requarter(v[3 * side][k, 8 * side : 8 * side + 8], k, base)
                acc = part if acc is None else jnp.where(quarter == k, part, acc)
            send_x[r, side] = acc
        for side, face in ((0, lower), (1, upper)):
            acc = None
            for k in range(c):
                part = jnp.where(b8 < 4, face[k, 0:8], turn(face[k, 8:16], 32, 1))
                part = turn(part, k + 5 * side, 0)
                acc = part if acc is None else jnp.where(y8 == k, part, acc)
            send_y[r, side] = acc
        lower = v[0]
        upper = turn(v[0], -7, 2)
        for t in range(1, 4):
            lower = jnp.where(node_c == t, turn(v[t], t, 2), lower)
            upper = jnp.where(node_c == t, turn(v[t], t - 7, 2), upper)
        for side, face in ((0, lower), (1, upper)):
            for k in range(c):
                send_z[r, side, k] = jnp.where(c8 < 4, face[k, 0:8], turn(face[k, 8:16], 4, 1))
        start(r, c)
        if hook is not None:
            hook()
        finish(r, c)
        for side in range(2):
            dx = 2 * side - 1
            low = turn(turn(z_joined(r, dx, -1), -56, 1), -3, 0)
            high = turn(turn(z_joined(r, dx, 1), 56, 1), 3, 0)
            face = z_joined(r, dx, 0) + jnp.where(
                (y8 == 0) & (b8 == 0), low, jnp.where((y8 == 3) & (b8 == 7), high, 0.0)
            )
            base = 3 * side
            parts = [
                jnp.where(quarter == base, requarter(face, k, base), 0.0) for k in range(c)
            ]
            part = jnp.stack(parts)
            zero = jnp.zeros_like(part)
            pair = [part, zero] if side == 0 else [zero, part]
            v[3 * side] = v[3 * side] + jnp.concatenate(pair, axis=1)
        got = []
        for side in range(2):
            face = z_joined(r, 0, 2 * side - 1)
            parts = []
            for k in range(c):
                part = jnp.where(y8 == 3 * side, turn(face, 3 * side - k, 0), 0.0)
                parts.append(jnp.concatenate([part, turn(part, -32, 1)], axis=0))
            got.append(jnp.stack(parts))
        add_y(got[0], got[1])
        got = []
        for side in range(2):
            face = recv_z[r, side, :c]
            got.append(jnp.concatenate([face, turn(face, -4, 2)], axis=1))
        for t in range(4):
            low, high = turn(got[0], -t, 2), turn(got[1], 7 - t, 2)
            v[t] = v[t] + jnp.where(node_c == 0, low, jnp.where(node_c == 7, high, 0.0))
        return v

    def advect(v):
        dx = along_x(0, v)
        dyz = along_lanes(v, fwd_ref)
        return [
            velocity[t][0:1] * dx[t]
            + velocity[t][1:2] * dyz[t][:, :, :128]
            + velocity[t][2:3] * dyz[t][:, :, 128:]
            for t in range(4)
        ]

    loads[3].wait()
    first = advect(velocity)
    diag = []
    mobile = []

    def diagonal():
        for load in loads[4:]:
            load.wait()
        dens = order(to_place, den_ref[...])
        mobile.extend(
            quad[t] * dens[:, 128 * t : 128 * t + 128].reshape(1, 16, 128) for t in range(4)
        )
        square_x = along_x(64, mobile)
        square_yz = along_lanes(mobile, sqr_ref)
        diag.extend(mass_shift * quad[t] + square_x[t] + square_yz[t] for t in range(4))

    pl.semaphore_wait(barrier, others)
    first = assemble(first, 0, diagonal)
    k1 = [first[t] * share[t] for t in range(4)]
    total_rate = k1
    v = [velocity[t] - (0.5 * time_step) * k1[t] for t in range(4)]
    for r, step, weight in ((1, 0.5, 2.0), (2, 1.0, 2.0), (3, 0.0, 1.0)):
        g = advect(v)
        if r == 1:
            g = assemble([jnp.concatenate([g[t], diag[t]], axis=0) for t in range(4)], r)
            inverse_jacobi = [1.0 / g[t][3:4] for t in range(4)]
            g = [g[t][0:3] for t in range(4)]
        else:
            g = assemble(g, r)
        g = [g[t] * share[t] for t in range(4)]
        total_rate = [total_rate[t] + weight * g[t] for t in range(4)]
        if step:
            v = [velocity[t] - (step * time_step) * g[t] for t in range(4)]
    advected = [velocity[t] - (time_step / 6.0) * total_rate[t] for t in range(4)]

    dx = along_x(0, [advected[t][0:1] for t in range(4)])
    dyz = along_lanes([advected[t][1:3] for t in range(4)], fwd_ref)
    div = [dx[t] + dyz[t][0:1, :, :128] + dyz[t][1:2, :, 128:] for t in range(4)]
    def put(field):
        return order(to_slot, field)

    def put_advected():
        for i in range(3):
            adv_ref[i] = put(jnp.concatenate([advected[t][i] for t in range(4)], axis=1))

    total_div = assemble(div, 4, put_advected)
    r0 = [total_div[t] * (quad[t] * (-1.0 / time_step)) for t in range(4)]

    def local(v):
        dx = along_x(0, v)
        dyz = along_lanes(v, fwd_ref)
        gx = [mobile[t] * dx[t] for t in range(4)]
        gyz = [
            jnp.concatenate(
                [mobile[t] * dyz[t][:, :, :128], mobile[t] * dyz[t][:, :, 128:]], axis=2
            )
            for t in range(4)
        ]
        bx = along_x(32, gx)
        byz = along_lanes(gyz, bwd_ref)
        return [(mass_shift * quad[t]) * v[t] + bx[t] + byz[t] for t in range(4)]

    def dot_row(a, b, scale=None):
        acc = None
        for t in range(4):
            term = a[t] * b[t]
            if scale is not None:
                term = term * scale[t]
            acc = term if acc is None else acc + term
        return jnp.sum(acc[0], axis=0, keepdims=True)

    z0 = [r0[t] * inverse_jacobi[t] for t in range(4)]
    lz = local(z0)
    rho_row = dot_row(r0, z0, share)
    gamma_row = dot_row(z0, lz)
    s = assemble(lz, 5)
    w = [s[t] * inverse_jacobi[t] for t in range(4)]
    lw = local(w)
    delta_row = dot_row(s, w, share)
    eps_row = dot_row(w, lw)
    partial = jnp.concatenate(
        [rho_row, gamma_row, delta_row, eps_row, jnp.zeros((4, 128), f32)], axis=0
    )
    partial = jnp.sum(partial, axis=1, keepdims=True)
    own = jnp.sum(jnp.where(sub8 == lane8, partial, 0.0), axis=0, keepdims=True)
    sums[...] = own

    def share_sums(device, index):
        pltpu.make_async_remote_copy(
            src_ref=sums,
            dst_ref=sums_in.at[index],
            send_sem=sum_send,
            recv_sem=sum_recv,
            device_id=device,
            device_id_type=MESH,
        ).start()

    each_other(share_sums)
    t_vec = assemble(lw, 6)
    arrived = pltpu.make_async_remote_copy(
        src_ref=sums_in,
        dst_ref=sums_in,
        send_sem=sum_send,
        recv_sem=sum_recv,
        device_id=tuple(lax.rem(me[i] + 1, counts[i]) for i in range(3)),
        device_id_type=MESH,
    )
    arrived.wait_recv()
    joined = own + jnp.sum(sums_in[...], axis=0)
    four = jnp.sum(jnp.where(sub8 == lane8, joined, 0.0), axis=1, keepdims=True)
    rho, gamma, delta, eps = (four[i : i + 1].reshape(1, 1, 1) for i in range(4))
    alpha0 = rho / gamma
    rho1 = rho - 2.0 * alpha0 * gamma + alpha0 * alpha0 * delta
    beta = rho1 / rho
    cross = gamma - alpha0 * delta
    curve = gamma - 2.0 * alpha0 * delta + alpha0 * alpha0 * eps
    curve = curve + 2.0 * beta * cross + beta * beta * gamma
    alpha1 = rho1 / curve
    along = alpha0 + alpha1 * (1.0 + beta)
    side_step = alpha0 * alpha1

    pre_ref[...] = put(
        jnp.concatenate([(along * z0[t] - side_step * w[t])[0] for t in range(4)], axis=1)
    )
    res_ref[...] = put(
        jnp.concatenate(
            [(r0[t] - along * s[t] + side_step * t_vec[t])[0] for t in range(4)], axis=1
        )
    )
    sent()
    arrived.wait_send()


def finish_kernel(adv_ref, pre_ref, res_ref, adv_out, pre_out, res_out):
    adv_out[...] = adv_ref[...]
    pre_out[...] = pre_ref[...]
    res_out[...] = res_ref[...]


def per_device(counts, velocity, inv_density, element_place):
    f32 = jnp.float32
    rows, forward, backward, square = constants()
    elements = element_place.shape[0]
    points = inv_density.shape[0]
    vmem = pl.BlockSpec(memory_space=pltpu.VMEM)
    faces = pltpu.VMEM((ROUNDS, 2, 8, 128), f32)
    faces_z = pltpu.VMEM((ROUNDS, 2, 4, 8, 128), f32)
    dma = pltpu.SemaphoreType.DMA
    others = counts[0] * counts[1] * counts[2] - 1
    shapes = (
        jax.ShapeDtypeStruct((3, elements, points), f32),
        jax.ShapeDtypeStruct((elements, points), f32),
        jax.ShapeDtypeStruct((elements, points), f32),
    )
    computed = pl.pallas_call(
        functools.partial(kernel, counts),
        out_shape=shapes,
        in_specs=[pl.BlockSpec(memory_space=pltpu.HBM)] * 7,
        out_specs=(vmem, vmem, vmem),
        scratch_shapes=[
            faces,
            faces,
            faces_z,
            pltpu.VMEM((ROUNDS, 27, 8, 128), f32),
            faces_z,
            pltpu.VMEM((1, 128), f32),
            pltpu.VMEM((others, 1, 128), f32),
            dma((11,)),
            dma((ROUNDS, 11)),
            dma,
            dma,
            pltpu.VMEM((3, elements, points), f32),
            pltpu.VMEM((elements, points), f32),
            pltpu.SMEM((elements,), jnp.int32),
            pltpu.VMEM(rows.shape, f32),
            pltpu.VMEM(forward.shape, jnp.bfloat16),
            pltpu.VMEM(backward.shape, jnp.bfloat16),
            pltpu.VMEM(square.shape, jnp.bfloat16),
            dma((7,)),
        ],
        compiler_params=pltpu.CompilerParams(
            collective_id=0, has_side_effects=True, vmem_limit_bytes=VMEM_LIMIT
        ),
    )(
        *(
            pltpu.with_memory_space_constraint(operand, pltpu.HBM)
            for operand in (
                velocity.transpose(0, 2, 1),
                inv_density.T,
                element_place,
                jnp.asarray(rows),
                jnp.asarray(forward),
                jnp.asarray(backward),
                jnp.asarray(square),
            )
        )
    )
    advected, pressure, residual = pl.pallas_call(
        finish_kernel,
        out_shape=shapes,
        in_specs=[vmem, vmem, vmem],
        out_specs=(vmem, vmem, vmem),
        compiler_params=pltpu.CompilerParams(vmem_limit_bytes=VMEM_LIMIT),
    )(*computed)
    return advected.transpose(0, 2, 1), pressure.T, residual.T


def solution(mesh):
    counts = tuple(mesh.shape[name] for name in AXES)
    placed = (P(None, None, AXES), P(None, AXES), P(AXES))
    return jax.shard_map(
        functools.partial(per_device, counts),
        mesh=mesh,
        in_specs=placed,
        out_specs=(P(None, None, AXES), P(None, AXES), P(None, AXES)),
        check_vma=False,
    )
```

```python
import functools

import jax
import jax.numpy as jnp
import numpy as np
from jax import lax
from jax.experimental import pallas as pl
from jax.experimental.pallas import tpu as pltpu
from jax.sharding import PartitionSpec as P

BX = 4
BY = 4
BZ = 1
MESH = pl.DeviceIdType.MESH
AXES = ("gx", "gy", "gz")
ROUNDS = 7
VMEM_LIMIT = 16 << 20

time_step = 0.03
mass_shift = 4.0
inner_nodes = (
    -0.8717401485096066,
    -0.5917001814331423,
    -0.2092992179024789,
    0.2092992179024789,
    0.5917001814331423,
    0.8717401485096066,
)


def legendre_seven(position):
    previous = 1.0
    current_value = position
    for degree_index in range(1, 7):
        following = (
            (2 * degree_index + 1) * position * current_value - degree_index * previous
        ) / (degree_index + 1)
        previous = current_value
        current_value = following
    return current_value


def tables():
    nodes = [-1.0] + list(inner_nodes) + [1.0]
    poly = [legendre_seven(node) for node in nodes]
    weights = np.array([2.0 / (56.0 * value * value) for value in poly])
    derivative = np.zeros((8, 8))
    for i in range(8):
        for j in range(8):
            if i != j:
                derivative[i, j] = poly[i] / (poly[j] * (nodes[i] - nodes[j]))
    derivative[0, 0] = -14.0
    derivative[7, 7] = 14.0
    return weights, derivative.astype(np.float32).astype(np.float64)


def split_stack(matrix):
    high = np.asarray(matrix, np.float32).astype(jnp.bfloat16)
    low = (np.asarray(matrix, np.float32) - high.astype(np.float32)).astype(jnp.bfloat16)
    return np.concatenate([high, high, low], axis=0)


LANE_NODES = (0, 2, 4, 6, 1, 3, 5, 7)


@functools.cache
def constants():
    weights, d = tables()
    nodes = list(LANE_NODES)
    eye16 = np.eye(16)

    def lanes(matrix):
        return split_stack(np.kron(matrix[np.ix_(nodes, nodes)], eye16))

    plane = np.outer(weights, np.repeat(weights[nodes], 16))
    return plane.astype(np.float32), lanes(d.T), lanes(d), lanes(d**2)


def along_index(matrix, sign, v):
    plus = [v[j] + v[7 - j] for j in range(4)]
    minus = [v[j] - v[7 - j] for j in range(4)]
    out = [None] * 8
    for i in range(4):
        even = odd = None
        for j in range(4):
            p = float(0.5 * (matrix[i, j] + matrix[i, 7 - j])) * plus[j]
            n = float(0.5 * (matrix[i, j] - matrix[i, 7 - j])) * minus[j]
            even = p if even is None else even + p
            odd = n if odd is None else odd + n
        out[i] = even + odd
        out[7 - i] = even - odd if sign > 0 else odd - even
    return out


def kernel(
    counts,
    vel_hbm,
    den_hbm,
    place_hbm,
    plane_hbm,
    fwd_hbm,
    bwd_hbm,
    sqr_hbm,
    adv_ref,
    pre_ref,
    res_ref,
    send_x,
    send_y,
    send_z,
    send_e,
    recv_xy,
    recv_z,
    recv_e,
    work_v,
    work_d,
    work_g,
    work_c,
    sums,
    sums_in,
    send_sem,
    recv_sem,
    sum_send,
    sum_recv,
    vel_ref,
    den_ref,
    place_ref,
    plane_ref,
    fwd_ref,
    bwd_ref,
    sqr_ref,
    load_sem,
):
    f32 = jnp.float32
    loads = [
        pltpu.make_async_copy(source_ref, target_ref, load_sem.at[index])
        for index, (source_ref, target_ref) in enumerate(
            (
                (place_hbm, place_ref),
                (vel_hbm, vel_ref),
                (den_hbm, den_ref),
                (fwd_hbm, fwd_ref),
                (plane_hbm, plane_ref),
                (sqr_hbm, sqr_ref),
                (bwd_hbm, bwd_ref),
            )
        )
    ]
    for load in loads:
        load.start()
    me = [lax.axis_index(name) for name in AXES]
    has = [(me[i] > 0, me[i] < counts[i] - 1) for i in range(3)]
    weights, deriv = tables()
    deriv_t, squared_t = deriv.T, deriv.T**2

    def each_other(act):
        for kx in range(counts[0]):
            for ky in range(counts[1]):
                base = (kx * counts[1] + ky) * counts[2]
                first = 0 if base else 1

                def one(kz, _):
                    steps = (kx, ky, kz)
                    device = tuple(lax.rem(me[i] + steps[i], counts[i]) for i in range(3))
                    act(device, base + kz - 1)
                    return 0

                if counts[2] <= 8:
                    for kz in range(first, counts[2]):
                        one(kz, 0)
                else:
                    lax.fori_loop(first, counts[2], one, 0)

    directions = [
        (dx, dy, dz)
        for dx in (-1, 0, 1)
        for dy in (-1, 0, 1)
        for dz in (-1, 0, 1)
        if (dx, dy, dz) != (0, 0, 0)
    ]

    def exists(d):
        flag = None
        for i in range(3):
            if d[i]:
                here = has[i][1 if d[i] > 0 else 0]
                flag = here if flag is None else jnp.logical_and(flag, here)
        return flag

    peers = {d: (exists(d), tuple(me[i] + d[i] for i in range(3))) for d in directions}
    order_out = sorted(directions, key=lambda d: -sum(abs(i) for i in d))

    barrier = pltpu.get_barrier_semaphore()

    def greet(device, index):
        pl.semaphore_signal(barrier, inc=1, device_id=device, device_id_type=MESH)

    if max(counts) <= ROUNDS:
        for d in directions:

            @pl.when(peers[d][0])
            def _():
                greet(peers[d][1], 0)

        greeted = 1
        for i in range(3):
            low, high = has[i]
            greeted = greeted * (1 + low.astype(jnp.int32) + high.astype(jnp.int32))
        others = greeted - 1
    else:
        each_other(greet)
        others = counts[0] * counts[1] * counts[2] - 1

    sub8 = lax.broadcasted_iota(jnp.int32, (8, 128), 0)
    lane8 = lax.broadcasted_iota(jnp.int32, (8, 128), 1)
    ex, ey = (lane8 // 4) % 4, lane8 % 4
    low_x, high_x = lane8 < 16, lane8 >= 112
    join_low_x, join_high_x = low_x & (ex > 0), high_x & (ex < 3)
    join_low_y, join_high_y = (sub8 == 0) & (ey > 0), (sub8 == 7) & (ey < 3)
    pack_b = lane8 // 16
    pack_low_y, pack_high_y = (pack_b == 0) & (ey > 0), (pack_b == 7) & (ey < 3)
    edge_low_y, edge_high_y = (pack_b == 0) & (ey == 0), (pack_b == 7) & (ey == 3)

    def half(flag):
        return jnp.where(flag, 0.5, 1.0).astype(f32)

    total = [BX * counts[0], BY * counts[1], BZ * counts[2]]
    pos_x, pos_y = ex + me[0] * BX, ey + me[1] * BY
    share_xy = half((low_x & (pos_x > 0)) | (high_x & (pos_x < total[0] - 1)))
    share_xy = share_xy * half(
        ((sub8 == 0) & (pos_y > 0)) | ((sub8 == 7) & (pos_y < total[1] - 1))
    )
    share_xy = share_xy.reshape(1, 8, 128)
    share = [share_xy] * 8
    share[0] = share_xy * half(has[2][0])
    share[7] = share_xy * half(has[2][1])

    def turn(x, shift, axis):
        size = x.shape[axis]
        shift = shift % size
        return pltpu.roll(x, shift, axis) if shift else x

    def rows_of(ref, count):
        return [
            jnp.stack([ref[k, pl.ds(b, 8, stride=8), :] for k in range(count)])
            for b in range(8)
        ]

    def planes_of(ref, count):
        return [
            jnp.stack([ref[k, 8 * c : 8 * c + 8, :] for k in range(count)]) for c in range(8)
        ]

    def put_rows(ref, rows):
        for b in range(8):
            for k in range(rows[b].shape[0]):
                ref[k, pl.ds(b, 8, stride=8), :] = rows[b][k]

    def put_planes(ref, planes):
        for c in range(8):
            for k in range(planes[c].shape[0]):
                ref[k, 8 * c : 8 * c + 8, :] = planes[c][k]

    loads[0].wait()
    r16 = lax.broadcasted_iota(jnp.int32, (16, 16), 0)
    l16 = lax.broadcasted_iota(jnp.int32, (16, 16), 1)
    by_lane = jnp.zeros((16, 16), jnp.int32)
    by_row = jnp.zeros((16, 16), jnp.int32)
    for e in range(16):
        by_lane = jnp.where(l16 == e, place_ref[e], by_lane)
        by_row = jnp.where(r16 == e, place_ref[e], by_row)
    to_place = (by_lane == r16).astype(f32)
    to_slot = (by_row == l16).astype(f32)

    def order(matrix, block):
        return jnp.dot(
            matrix, block, precision=lax.Precision.HIGHEST, preferred_element_type=f32
        )

    lane64 = lax.broadcasted_iota(jnp.int32, (64, 128), 1)

    def take(first, second):
        blocks = [
            order(to_place, field)[:, 128 * t : 128 * t + 128]
            for field in (first, second)
            for t in range(4)
        ]
        turned = jnp.concatenate(blocks, axis=0).T
        top, bottom = turned[:64], turned[64:]
        left = jnp.where(lane64 < 64, top, turn(bottom, 64, 1))
        right = jnp.where(lane64 < 64, turn(top, 64, 1), bottom)
        return left, right

    def give(first, second):
        for k, field in enumerate((first, second)):
            for c in range(8):
                work_d[k, 8 * c : 8 * c + 8, :] = field[c].reshape(8, 128)
        left, right = (
            jnp.concatenate(
                [work_d[k, pl.ds(b, 8, stride=8), :] for b in range(8)], axis=0
            )
            for k in range(2)
        )
        top = jnp.where(lane64 < 64, left, turn(right, 64, 1))
        bottom = jnp.where(lane64 < 64, turn(left, 64, 1), right)
        turned = jnp.concatenate([top, bottom], axis=0).T
        return [
            order(
                to_slot,
                jnp.concatenate(
                    [turned[64 * k + 16 * t : 64 * k + 16 * t + 16] for t in range(4)], axis=1
                ),
            )
            for k in range(2)
        ]

    loads[1].wait()
    loads[2].wait()
    taken = [*take(vel_ref[0], vel_ref[1]), *take(vel_ref[2], den_ref[...])]
    put_rows(
        work_v, [jnp.stack([f[8 * b : 8 * b + 8] for f in taken]) for b in range(8)]
    )
    planes = planes_of(work_v, 4)
    velocity = [planes[c][0:3] for c in range(8)]

    def split(x):
        high = x.astype(jnp.bfloat16)
        low = (x - high.astype(f32)).astype(jnp.bfloat16)
        return jnp.concatenate([high, low, high], axis=1)

    def along_x(v, w_ref):
        c = v[0].shape[0]
        x = jnp.concatenate([v[t].reshape(c * 8, 128) for t in range(8)], axis=0)
        y = jnp.dot(split(x), w_ref[...], preferred_element_type=f32)
        return [y[t * c * 8 : (t + 1) * c * 8].reshape(c, 8, 128) for t in range(8)]

    def along_y(v, matrix, sign):
        c = v[0].shape[0]
        put_planes(work_v, v)
        put_rows(work_d, along_index(matrix, sign, rows_of(work_v, c)))
        return planes_of(work_d, c)

    def code(d):
        return (d[0] + 1) * 9 + (d[1] + 1) * 3 + d[2] + 1

    def side_of(step):
        return 1 if step > 0 else 0

    def column(dx, dy):
        return 3 * (dx + 1) + dy + 1

    def source(r, d, c):
        if not d[0] and not d[1]:
            return send_z.at[r, side_of(d[2]), pl.ds(0, c)]
        if d[2]:
            base = 2 * side_of(d[0]) if d[0] else 4 + 2 * side_of(d[1])
            return send_e.at[r, base + side_of(d[2])]
        return (send_x if d[0] else send_y).at[r, side_of(d[0] if d[0] else d[1])]

    def target(r, d, c):
        if not d[0] and not d[1]:
            return recv_z.at[r, side_of(d[2]), pl.ds(0, c)]
        if d[2]:
            return recv_e.at[r, code(d)]
        return recv_xy.at[r, column(d[0], d[1])]

    def copy(r, d, c, incoming):
        back = d if incoming else tuple(-i for i in d)
        return pltpu.make_async_remote_copy(
            src_ref=source(r, d, c),
            dst_ref=target(r, back, c),
            send_sem=send_sem.at[code(d)],
            recv_sem=recv_sem.at[r, code(back)],
            device_id=peers[d][1],
            device_id_type=MESH,
        )

    def start(r, c):
        for d in order_out:

            @pl.when(peers[d][0])
            def _():
                copy(r, d, c, False).start()

    def finish(r, c):
        for d in order_out[::-1]:

            @pl.when(peers[d][0])
            def _():
                copy(r, d, c, True).wait_recv()

    def sent():
        for d in directions:
            if not d[0] and not d[1]:
                ref = recv_z.at[pl.ds(0, 2)]
            elif d[2]:
                ref = recv_e.at[:, 0]
            else:
                ref = recv_xy.at[:, 0]

            @pl.when(peers[d][0])
            def _():
                pltpu.make_async_remote_copy(
                    src_ref=ref,
                    dst_ref=ref,
                    send_sem=send_sem.at[code(d)],
                    recv_sem=recv_sem.at[0, code(d)],
                    device_id=peers[d][1],
                    device_id_type=MESH,
                ).wait_send()

    def clear():
        for d in directions:

            @pl.when(jnp.logical_not(peers[d][0]))
            def _():
                for r in range(ROUNDS):
                    if not d[0] and not d[1]:
                        recv_z[r, side_of(d[2])] = jnp.zeros((4, 8, 128), f32)
                    elif d[2]:
                        recv_e[r, code(d)] = jnp.zeros((1, 128), f32)
                    else:
                        recv_xy[r, column(d[0], d[1])] = jnp.zeros((8, 128), f32)

    def join_x(v):
        low, high = turn(v, 20, 2), turn(v, -20, 2)
        return v + jnp.where(join_low_x, low, jnp.where(join_high_x, high, 0.0))

    def join_y(v):
        low, high = turn(turn(v, 1, 1), 1, 2), turn(turn(v, -1, 1), -1, 2)
        return v + jnp.where(join_low_y, low, jnp.where(join_high_y, high, 0.0))

    def merge(parts, index, bit=1):
        while len(parts) > 1:
            parts = [
                jnp.where((index & bit) == 0, parts[i], parts[i + 1])
                for i in range(0, len(parts), 2)
            ]
            bit *= 2
        return parts[0]

    def z_joined(r, dx, dy):
        low, high = recv_e[r, code((dx, dy, -1))], recv_e[r, code((dx, dy, 1))]
        return recv_xy[r, column(dx, dy)] + jnp.where(
            sub8 == 0, low, jnp.where(sub8 == 7, high, 0.0)
        )

    def assemble(v, r, hook=None):
        c = v[0].shape[0]
        put_planes(work_g, v)
        rows = [
            [work_g[k, pl.ds(b, 8, stride=8), :] for k in range(c)] for b in range(8)
        ]
        for side in range(2):
            packed = []
            for b in range(8):
                acc = turn(rows[b][0], 16 * b - 124 * side, 1)
                for k in range(1, c):
                    part = turn(rows[b][k], 16 * b + 4 * k - 124 * side, 1)
                    acc = jnp.where(ex == k, part, acc)
                packed.append(acc)
            face = merge(packed, pack_b)
            low, high = turn(face, 17, 1), turn(face, -17, 1)
            face = face + jnp.where(pack_low_y, low, jnp.where(pack_high_y, high, 0.0))
            send_x[r, side] = face
            send_e[r, 2 * side] = face[0:1]
            send_e[r, 2 * side + 1] = face[7:8]
        for side in range(2):
            face = turn(rows[7 * side][0], -3 * side, 1)
            for k in range(1, c):
                face = jnp.where(ey == k, turn(rows[7 * side][k], k - 3 * side, 1), face)
            low, high = turn(face, 20, 1), turn(face, -20, 1)
            face = face + jnp.where(join_low_x, low, jnp.where(join_high_x, high, 0.0))
            send_y[r, side] = face
            send_e[r, 4 + 2 * side] = face[0:1]
            send_e[r, 5 + 2 * side] = face[7:8]
        v = list(v)
        for side in range(2):
            v[7 * side] = join_x(join_y(v[7 * side]))
            send_z[r, side, pl.ds(0, c)] = v[7 * side]
        start(r, c)
        for t in range(1, 7):
            v[t] = join_x(join_y(v[t]))
        if hook is not None:
            hook()
        finish(r, c)
        faces = []
        for dx in (-1, 1):
            low = turn(z_joined(r, dx, -1), 13, 1)
            high = turn(z_joined(r, dx, 1), -13, 1)
            faces.append(
                z_joined(r, dx, 0)
                + jnp.where(edge_low_y, low, jnp.where(edge_high_y, high, 0.0))
            )
        for b in range(8):
            for k in range(c):
                low = turn(faces[0], -16 * b - 4 * k, 1)
                high = turn(faces[1], 124 - 16 * b - 4 * k, 1)
                part = jnp.where(lane8 < 4, low, jnp.where(lane8 >= 124, high, 0.0))
                if b in (0, 7):
                    near = 3 if b else 0
                    face = turn(z_joined(r, 0, 1 if b else -1), near - k, 1)
                    part = part + jnp.where(ey == near, face, 0.0)
                work_c[k, pl.ds(b, 8, stride=8), :] = part
        corrections = planes_of(work_c, c)
        v = [v[t] + corrections[t] for t in range(8)]
        for side in range(2):
            v[7 * side] = v[7 * side] + recv_z[r, side, :c]
        return v

    def advect(v):
        dx = along_x(v, fwd_ref)
        dy = along_y(v, deriv, -1)
        dz = along_index(deriv, -1, v)
        return [
            velocity[t][0:1] * dx[t] + velocity[t][1:2] * dy[t] + velocity[t][2:3] * dz[t]
            for t in range(8)
        ]

    loads[3].wait()
    first = advect(velocity)
    diag, quad, mobile = [], [], []

    def diagonal():
        clear()
        for load in loads[4:]:
            load.wait()
        plane = plane_ref[...].reshape(1, 8, 128)
        quad.extend(plane * float(weights[t]) for t in range(8))
        mobile.extend(quad[t] * planes[t][3:4] for t in range(8))
        square_x = along_x(mobile, sqr_ref)
        square_y = along_y(mobile, squared_t, 1)
        square_z = along_index(squared_t, 1, mobile)
        diag.extend(
            mass_shift * quad[t] + square_x[t] + square_y[t] + square_z[t] for t in range(8)
        )

    pl.semaphore_wait(barrier, others)
    first = assemble(first, 0, diagonal)
    k1 = [first[t] * share[t] for t in range(8)]
    total_rate = k1
    v = [velocity[t] - (0.5 * time_step) * k1[t] for t in range(8)]
    for r, step, weight in ((1, 0.5, 2.0), (2, 1.0, 2.0), (3, 0.0, 1.0)):
        g = advect(v)
        if r == 1:
            g = assemble([jnp.concatenate([g[t], diag[t]], axis=0) for t in range(8)], r)
            inverse_jacobi = [1.0 / g[t][3:4] for t in range(8)]
            g = [g[t][0:3] for t in range(8)]
        else:
            g = assemble(g, r)
        g = [g[t] * share[t] for t in range(8)]
        total_rate = [total_rate[t] + weight * g[t] for t in range(8)]
        if step:
            v = [velocity[t] - (step * time_step) * g[t] for t in range(8)]
    advected = [velocity[t] - (time_step / 6.0) * total_rate[t] for t in range(8)]

    div_x = along_x([advected[t][0:1] for t in range(8)], fwd_ref)
    div_y = along_y([advected[t][1:2] for t in range(8)], deriv, -1)
    div_z = along_index(deriv, -1, [advected[t][2:3] for t in range(8)])
    div = [div_x[t] + div_y[t] + div_z[t] for t in range(8)]

    def put_advected():
        parts = [[advected[t][i] for t in range(8)] for i in range(3)]
        adv_ref[0], adv_ref[1] = give(parts[0], parts[1])
        adv_ref[2], _ = give(parts[2], parts[2])

    total_div = assemble(div, 4, put_advected)
    r0 = [total_div[t] * (quad[t] * (-1.0 / time_step)) for t in range(8)]

    def local(v):
        dx = along_x(v, fwd_ref)
        dy = along_y(v, deriv, -1)
        dz = along_index(deriv, -1, v)
        bx = along_x([mobile[t] * dx[t] for t in range(8)], bwd_ref)
        by = along_y([mobile[t] * dy[t] for t in range(8)], deriv_t, -1)
        bz = along_index(deriv_t, -1, [mobile[t] * dz[t] for t in range(8)])
        return [(mass_shift * quad[t]) * v[t] + bx[t] + by[t] + bz[t] for t in range(8)]

    def dot_row(a, b, scale=None):
        acc = None
        for t in range(8):
            term = a[t] * b[t]
            if scale is not None:
                term = term * scale[t]
            acc = term if acc is None else acc + term
        return jnp.sum(acc[0], axis=0, keepdims=True)

    given = {}

    def give_first():
        given["r0"], given["z0"] = give(r0, z0)

    def give_second():
        given["s"], given["w"] = give(s, w)

    z0 = [r0[t] * inverse_jacobi[t] for t in range(8)]
    lz = local(z0)
    rho_row = dot_row(r0, z0, share)
    gamma_row = dot_row(z0, lz)
    s = assemble(lz, 5, give_first)
    w = [s[t] * inverse_jacobi[t] for t in range(8)]
    lw = local(w)
    delta_row = dot_row(s, w, share)
    eps_row = dot_row(w, lw)
    partial = jnp.concatenate(
        [rho_row, gamma_row, delta_row, eps_row, jnp.zeros((4, 128), f32)], axis=0
    )
    partial = jnp.sum(partial, axis=1, keepdims=True)
    own = jnp.sum(jnp.where(sub8 == lane8, partial, 0.0), axis=0, keepdims=True)
    sums[...] = own

    def share_sums(device, index):
        pltpu.make_async_remote_copy(
            src_ref=sums,
            dst_ref=sums_in.at[index],
            send_sem=sum_send,
            recv_sem=sum_recv,
            device_id=device,
            device_id_type=MESH,
        ).start()

    each_other(share_sums)
    t_vec = assemble(lw, 6, give_second)
    third, _ = give(t_vec, t_vec)
    arrived = pltpu.make_async_remote_copy(
        src_ref=sums_in,
        dst_ref=sums_in,
        send_sem=sum_send,
        recv_sem=sum_recv,
        device_id=tuple(lax.rem(me[i] + 1, counts[i]) for i in range(3)),
        device_id_type=MESH,
    )
    arrived.wait_recv()
    joined = own + jnp.sum(sums_in[...], axis=0)
    four = jnp.sum(jnp.where(sub8 == lane8, joined, 0.0), axis=1, keepdims=True)
    rho, gamma, delta, eps = (four[i : i + 1] for i in range(4))
    alpha0 = rho / gamma
    rho1 = rho - 2.0 * alpha0 * gamma + alpha0 * alpha0 * delta
    beta = rho1 / rho
    cross = gamma - alpha0 * delta
    curve = gamma - 2.0 * alpha0 * delta + alpha0 * alpha0 * eps
    curve = curve + 2.0 * beta * cross + beta * beta * gamma
    alpha1 = rho1 / curve
    along = alpha0 + alpha1 * (1.0 + beta)
    side_step = alpha0 * alpha1

    pre_ref[...] = along * given["z0"] - side_step * given["w"]
    res_ref[...] = given["r0"] - along * given["s"] + side_step * third
    sent()
    arrived.wait_send()


def finish_kernel(adv_ref, pre_ref, res_ref, adv_out, pre_out, res_out):
    adv_out[...] = adv_ref[...]
    pre_out[...] = pre_ref[...]
    res_out[...] = res_ref[...]


def per_device(counts, velocity, inv_density, element_place):
    f32 = jnp.float32
    plane, forward, backward, square = constants()
    elements = element_place.shape[0]
    points = inv_density.shape[0]
    vmem = pl.BlockSpec(memory_space=pltpu.VMEM)
    faces = pltpu.VMEM((ROUNDS, 2, 8, 128), f32)
    faces_z = pltpu.VMEM((ROUNDS, 2, 4, 8, 128), f32)
    work = pltpu.VMEM((4, 64, 128), f32)
    dma = pltpu.SemaphoreType.DMA
    others = counts[0] * counts[1] * counts[2] - 1
    shapes = (
        jax.ShapeDtypeStruct((3, elements, points), f32),
        jax.ShapeDtypeStruct((elements, points), f32),
        jax.ShapeDtypeStruct((elements, points), f32),
    )
    computed = pl.pallas_call(
        functools.partial(kernel, counts),
        out_shape=shapes,
        in_specs=[pl.BlockSpec(memory_space=pltpu.HBM)] * 7,
        out_specs=(vmem, vmem, vmem),
        scratch_shapes=[
            faces,
            faces,
            faces_z,
            pltpu.VMEM((ROUNDS, 8, 1, 128), f32),
            pltpu.VMEM((ROUNDS, 9, 8, 128), f32),
            faces_z,
            pltpu.VMEM((ROUNDS, 27, 1, 128), f32),
            work,
            work,
            work,
            work,
            pltpu.VMEM((1, 128), f32),
            pltpu.VMEM((others, 1, 128), f32),
            dma((27,)),
            dma((ROUNDS, 27)),
            dma,
            dma,
            pltpu.VMEM((3, elements, points), f32),
            pltpu.VMEM((elements, points), f32),
            pltpu.SMEM((elements,), jnp.int32),
            pltpu.VMEM(plane.shape, f32),
            pltpu.VMEM(forward.shape, jnp.bfloat16),
            pltpu.VMEM(backward.shape, jnp.bfloat16),
            pltpu.VMEM(square.shape, jnp.bfloat16),
            dma((7,)),
        ],
        compiler_params=pltpu.CompilerParams(
            collective_id=0, has_side_effects=True, vmem_limit_bytes=VMEM_LIMIT
        ),
    )(
        *(
            pltpu.with_memory_space_constraint(operand, pltpu.HBM)
            for operand in (
                velocity.transpose(0, 2, 1),
                inv_density.T,
                element_place,
                jnp.asarray(plane),
                jnp.asarray(forward),
                jnp.asarray(backward),
                jnp.asarray(square),
            )
        )
    )
    advected, pressure, residual = pl.pallas_call(
        finish_kernel,
        out_shape=shapes,
        in_specs=[vmem, vmem, vmem],
        out_specs=(vmem, vmem, vmem),
        compiler_params=pltpu.CompilerParams(vmem_limit_bytes=VMEM_LIMIT),
    )(*computed)
    return advected.transpose(0, 2, 1), pressure.T, residual.T


def solution(mesh):
    counts = tuple(mesh.shape[name] for name in AXES)
    placed = (P(None, None, AXES), P(None, AXES), P(AXES))
    return jax.shard_map(
        functools.partial(per_device, counts),
        mesh=mesh,
        in_specs=placed,
        out_specs=(P(None, None, AXES), P(None, AXES), P(None, AXES)),
        check_vma=False,
    )
```

```python
import functools

import jax
import jax.numpy as jnp
import numpy as np
from jax import lax
from jax.experimental import pallas as pl
from jax.experimental.pallas import tpu as pltpu
from jax.sharding import PartitionSpec as P

BX = 4
BY = 4
BZ = 1
MESH = pl.DeviceIdType.MESH
AXES = ("gx", "gy", "gz")
ROUNDS = 7
VMEM_LIMIT = 16 << 20

time_step = 0.03
mass_shift = 4.0
inner_nodes = (
    -0.8717401485096066,
    -0.5917001814331423,
    -0.2092992179024789,
    0.2092992179024789,
    0.5917001814331423,
    0.8717401485096066,
)


def legendre_seven(position):
    previous = 1.0
    current_value = position
    for degree_index in range(1, 7):
        following = (
            (2 * degree_index + 1) * position * current_value - degree_index * previous
        ) / (degree_index + 1)
        previous = current_value
        current_value = following
    return current_value


def tables():
    nodes = [-1.0] + list(inner_nodes) + [1.0]
    poly = [legendre_seven(node) for node in nodes]
    weights = np.array([2.0 / (56.0 * value * value) for value in poly])
    derivative = np.zeros((8, 8))
    for i in range(8):
        for j in range(8):
            if i != j:
                derivative[i, j] = poly[i] / (poly[j] * (nodes[i] - nodes[j]))
    derivative[0, 0] = -14.0
    derivative[7, 7] = 14.0
    return weights, derivative.astype(np.float32).astype(np.float64)


def split_stack(matrix):
    high = np.asarray(matrix, np.float32).astype(jnp.bfloat16)
    low = (np.asarray(matrix, np.float32) - high.astype(np.float32)).astype(jnp.bfloat16)
    return np.concatenate([high, high, low], axis=0)


LANE_NODES = (0, 2, 4, 6, 1, 3, 5, 7)


@functools.cache
def constants():
    weights, d = tables()
    nodes = list(LANE_NODES)
    eye16 = np.eye(16)

    def lanes(matrix):
        return split_stack(np.kron(matrix[np.ix_(nodes, nodes)], eye16))

    plane = np.outer(weights, np.repeat(weights[nodes], 16))
    return plane.astype(np.float32), lanes(d.T), lanes(d), lanes(d**2)


def along_index(matrix, sign, v):
    plus = [v[j] + v[7 - j] for j in range(4)]
    minus = [v[j] - v[7 - j] for j in range(4)]
    out = [None] * 8
    for i in range(4):
        even = odd = None
        for j in range(4):
            p = float(0.5 * (matrix[i, j] + matrix[i, 7 - j])) * plus[j]
            n = float(0.5 * (matrix[i, j] - matrix[i, 7 - j])) * minus[j]
            even = p if even is None else even + p
            odd = n if odd is None else odd + n
        out[i] = even + odd
        out[7 - i] = even - odd if sign > 0 else odd - even
    return out


def kernel(
    counts,
    vel_hbm,
    den_hbm,
    place_hbm,
    plane_hbm,
    fwd_hbm,
    bwd_hbm,
    sqr_hbm,
    adv_ref,
    pre_ref,
    res_ref,
    send_x,
    send_y,
    send_z,
    send_e,
    recv_xy,
    recv_z,
    recv_e,
    work_v,
    work_d,
    work_g,
    work_c,
    sums,
    sums_in,
    send_sem,
    recv_sem,
    sum_send,
    sum_recv,
    vel_ref,
    den_ref,
    place_ref,
    plane_ref,
    fwd_ref,
    bwd_ref,
    sqr_ref,
    load_sem,
):
    f32 = jnp.float32
    loads = [
        pltpu.make_async_copy(source_ref, target_ref, load_sem.at[index])
        for index, (source_ref, target_ref) in enumerate(
            (
                (place_hbm, place_ref),
                (vel_hbm, vel_ref),
                (den_hbm, den_ref),
                (fwd_hbm, fwd_ref),
                (plane_hbm, plane_ref),
                (sqr_hbm, sqr_ref),
                (bwd_hbm, bwd_ref),
            )
        )
    ]
    for load in loads:
        load.start()
    me = [lax.axis_index(name) for name in AXES]
    has = [(me[i] > 0, me[i] < counts[i] - 1) for i in range(3)]
    weights, deriv = tables()
    deriv_t, squared_t = deriv.T, deriv.T**2

    def each_other(act):
        for kx in range(counts[0]):
            for ky in range(counts[1]):
                base = (kx * counts[1] + ky) * counts[2]
                first = 0 if base else 1

                def one(kz, _):
                    steps = (kx, ky, kz)
                    device = tuple(lax.rem(me[i] + steps[i], counts[i]) for i in range(3))
                    act(device, base + kz - 1)
                    return 0

                if counts[2] <= 8:
                    for kz in range(first, counts[2]):
                        one(kz, 0)
                else:
                    lax.fori_loop(first, counts[2], one, 0)

    directions = [
        (dx, dy, dz)
        for dx in (-1, 0, 1)
        for dy in (-1, 0, 1)
        for dz in (-1, 0, 1)
        if (dx, dy, dz) != (0, 0, 0)
    ]

    def exists(d):
        flag = None
        for i in range(3):
            if d[i]:
                here = has[i][1 if d[i] > 0 else 0]
                flag = here if flag is None else jnp.logical_and(flag, here)
        return flag

    peers = {d: (exists(d), tuple(me[i] + d[i] for i in range(3))) for d in directions}
    far = [d for d in directions if d[1] and d[2]]
    far.sort(key=lambda d: abs(d[0]))
    near_edges = [d for d in directions if d[0] and d[2] and not d[1]]
    near = [d for d in directions if d not in far and d not in near_edges]
    near.sort(key=lambda d: (-abs(d[2]), -abs(d[1]), abs(d[0])))

    barrier = pltpu.get_barrier_semaphore()

    def greet(device, index):
        pl.semaphore_signal(barrier, inc=1, device_id=device, device_id_type=MESH)

    if max(counts) <= ROUNDS:
        for d in directions:

            @pl.when(peers[d][0])
            def _():
                greet(peers[d][1], 0)

        greeted = 1
        for i in range(3):
            low, high = has[i]
            greeted = greeted * (1 + low.astype(jnp.int32) + high.astype(jnp.int32))
        others = greeted - 1
    else:
        each_other(greet)
        others = counts[0] * counts[1] * counts[2] - 1

    sub8 = lax.broadcasted_iota(jnp.int32, (8, 128), 0)
    lane8 = lax.broadcasted_iota(jnp.int32, (8, 128), 1)
    ex, ey = (lane8 // 4) % 4, lane8 % 4
    low_x, high_x = lane8 < 16, lane8 >= 112
    join_low_x, join_high_x = low_x & (ex > 0), high_x & (ex < 3)
    join_low_y, join_high_y = (sub8 == 0) & (ey > 0), (sub8 == 7) & (ey < 3)
    pack_b = lane8 // 16
    pack_low_y, pack_high_y = (pack_b == 0) & (ey > 0), (pack_b == 7) & (ey < 3)
    edge_low_y, edge_high_y = (pack_b == 0) & (ey == 0), (pack_b == 7) & (ey == 3)

    def half(flag):
        return jnp.where(flag, 0.5, 1.0).astype(f32)

    total = [BX * counts[0], BY * counts[1], BZ * counts[2]]
    pos_x, pos_y = ex + me[0] * BX, ey + me[1] * BY
    share_xy = half((low_x & (pos_x > 0)) | (high_x & (pos_x < total[0] - 1)))
    share_xy = share_xy * half(
        ((sub8 == 0) & (pos_y > 0)) | ((sub8 == 7) & (pos_y < total[1] - 1))
    )
    share_xy = share_xy.reshape(1, 8, 128)
    share = [share_xy] * 8
    share[0] = share_xy * half(has[2][0])
    share[7] = share_xy * half(has[2][1])

    def turn(x, shift, axis):
        size = x.shape[axis]
        shift = shift % size
        return pltpu.roll(x, shift, axis) if shift else x

    def rows_of(ref, count):
        return [
            jnp.stack([ref[k, pl.ds(b, 8, stride=8), :] for k in range(count)])
            for b in range(8)
        ]

    def planes_of(ref, count):
        return [
            jnp.stack([ref[k, 8 * c : 8 * c + 8, :] for k in range(count)]) for c in range(8)
        ]

    def put_rows(ref, rows):
        for b in range(8):
            for k in range(rows[b].shape[0]):
                ref[k, pl.ds(b, 8, stride=8), :] = rows[b][k]

    def put_planes(ref, planes):
        for c in range(8):
            for k in range(planes[c].shape[0]):
                ref[k, 8 * c : 8 * c + 8, :] = planes[c][k]

    loads[0].wait()
    r16 = lax.broadcasted_iota(jnp.int32, (16, 16), 0)
    l16 = lax.broadcasted_iota(jnp.int32, (16, 16), 1)
    by_lane = jnp.zeros((16, 16), jnp.int32)
    by_row = jnp.zeros((16, 16), jnp.int32)
    for e in range(16):
        by_lane = jnp.where(l16 == e, place_ref[e], by_lane)
        by_row = jnp.where(r16 == e, place_ref[e], by_row)
    to_place = (by_lane == r16).astype(f32)
    to_slot = (by_row == l16).astype(f32)

    def order(matrix, block):
        return jnp.dot(
            matrix, block, precision=lax.Precision.HIGHEST, preferred_element_type=f32
        )

    lane64 = lax.broadcasted_iota(jnp.int32, (64, 128), 1)

    def take(first, second):
        blocks = [
            order(to_place, field)[:, 128 * t : 128 * t + 128]
            for field in (first, second)
            for t in range(4)
        ]
        turned = jnp.concatenate(blocks, axis=0).T
        top, bottom = turned[:64], turned[64:]
        left = jnp.where(lane64 < 64, top, turn(bottom, 64, 1))
        right = jnp.where(lane64 < 64, turn(top, 64, 1), bottom)
        return left, right

    def give(first, second):
        for k, field in enumerate((first, second)):
            for c in range(8):
                work_d[k, 8 * c : 8 * c + 8, :] = field[c].reshape(8, 128)
        left, right = (
            jnp.concatenate(
                [work_d[k, pl.ds(b, 8, stride=8), :] for b in range(8)], axis=0
            )
            for k in range(2)
        )
        top = jnp.where(lane64 < 64, left, turn(right, 64, 1))
        bottom = jnp.where(lane64 < 64, turn(left, 64, 1), right)
        turned = jnp.concatenate([top, bottom], axis=0).T
        return [
            order(
                to_slot,
                jnp.concatenate(
                    [turned[64 * k + 16 * t : 64 * k + 16 * t + 16] for t in range(4)], axis=1
                ),
            )
            for k in range(2)
        ]

    loads[1].wait()
    loads[2].wait()
    taken = [*take(vel_ref[0], vel_ref[1]), *take(vel_ref[2], den_ref[...])]
    put_rows(
        work_v, [jnp.stack([f[8 * b : 8 * b + 8] for f in taken]) for b in range(8)]
    )
    planes = planes_of(work_v, 4)
    velocity = [planes[c][0:3] for c in range(8)]

    def split(x):
        high = x.astype(jnp.bfloat16)
        low = (x - high.astype(f32)).astype(jnp.bfloat16)
        return jnp.concatenate([high, low, high], axis=1)

    def along_x(v, w_ref):
        c = v[0].shape[0]
        x = jnp.concatenate([v[t].reshape(c * 8, 128) for t in range(8)], axis=0)
        y = jnp.dot(split(x), w_ref[...], preferred_element_type=f32)
        return [y[t * c * 8 : (t + 1) * c * 8].reshape(c, 8, 128) for t in range(8)]

    def along_y(v, matrix, sign):
        c = v[0].shape[0]
        put_planes(work_v, v)
        put_rows(work_d, along_index(matrix, sign, rows_of(work_v, c)))
        return planes_of(work_d, c)

    def code(d):
        return (d[0] + 1) * 9 + (d[1] + 1) * 3 + d[2] + 1

    def side_of(step):
        return 1 if step > 0 else 0

    def column(dx, dy):
        return 3 * (dx + 1) + dy + 1

    def source(r, d, c):
        if not d[0] and not d[1]:
            return send_z.at[r, side_of(d[2]), pl.ds(0, c)]
        if d[2]:
            kind = (8 if d[1] else 0) if d[0] else 4
            return send_e.at[r, kind + 2 * side_of(d[0] or d[1]) + side_of(d[2])]
        return (send_x if d[0] else send_y).at[r, side_of(d[0] if d[0] else d[1])]

    def target(r, d, c):
        if not d[0] and not d[1]:
            return recv_z.at[r, side_of(d[2]), pl.ds(0, c)]
        if d[2]:
            return recv_e.at[r, code(d)]
        return recv_xy.at[r, column(d[0], d[1])]

    def copy(r, d, c, incoming):
        back = d if incoming else tuple(-i for i in d)
        return pltpu.make_async_remote_copy(
            src_ref=source(r, d, c),
            dst_ref=target(r, back, c),
            send_sem=send_sem.at[code(d)],
            recv_sem=recv_sem.at[r, code(back)],
            device_id=peers[d][1],
            device_id_type=MESH,
        )

    def start(r, c, group):
        for d in group:

            @pl.when(peers[d][0])
            def _():
                copy(r, d, c, False).start()

    def finish(r, c, group):
        for d in group[::-1]:

            @pl.when(peers[d][0])
            def _():
                copy(r, d, c, True).wait_recv()

    def sent():
        for d in directions:
            if not d[0] and not d[1]:
                ref = recv_z.at[pl.ds(0, 2)]
            elif d[2]:
                ref = recv_e.at[:, 0]
            else:
                ref = recv_xy.at[:, 0]

            @pl.when(peers[d][0])
            def _():
                pltpu.make_async_remote_copy(
                    src_ref=ref,
                    dst_ref=ref,
                    send_sem=send_sem.at[code(d)],
                    recv_sem=recv_sem.at[0, code(d)],
                    device_id=peers[d][1],
                    device_id_type=MESH,
                ).wait_send()

    def clear():
        for d in directions:

            @pl.when(jnp.logical_not(peers[d][0]))
            def _():
                for r in range(ROUNDS):
                    if not d[0] and not d[1]:
                        recv_z[r, side_of(d[2])] = jnp.zeros((4, 8, 128), f32)
                    elif d[2]:
                        recv_e[r, code(d)] = jnp.zeros((1, 128), f32)
                    else:
                        recv_xy[r, column(d[0], d[1])] = jnp.zeros((8, 128), f32)

    def join_x(v):
        low, high = turn(v, 20, 2), turn(v, -20, 2)
        return v + jnp.where(join_low_x, low, jnp.where(join_high_x, high, 0.0))

    def join_y(v):
        low, high = turn(turn(v, 1, 1), 1, 2), turn(turn(v, -1, 1), -1, 2)
        return v + jnp.where(join_low_y, low, jnp.where(join_high_y, high, 0.0))

    def merge(parts, index, bit=1):
        while len(parts) > 1:
            parts = [
                jnp.where((index & bit) == 0, parts[i], parts[i + 1])
                for i in range(0, len(parts), 2)
            ]
            bit *= 2
        return parts[0]

    def by_slot(parts, slot):
        acc = parts[0]
        for k in range(1, len(parts)):
            acc = jnp.where(slot == k, parts[k], acc)
        return acc

    def edge_rows(r, dx, dy):
        low, high = recv_e[r, code((dx, dy, -1))], recv_e[r, code((dx, dy, 1))]
        return jnp.where(sub8 == 0, low, jnp.where(sub8 == 7, high, 0.0))

    def assemble(v, r, hook=None):
        c = v[0].shape[0]
        put_planes(work_g, v)
        rows = [
            [work_g[k, pl.ds(b, 8, stride=8), :] for k in range(c)] for b in range(8)
        ]
        for side in range(2):
            own = rows[7 * side]
            face = by_slot([turn(own[k], k - 3 * side, 1) for k in range(c)], ey)
            low = by_slot([turn(own[k], k - 3 * side + 20, 1) for k in range(c)], ey)
            high = by_slot([turn(own[k], k - 3 * side - 20, 1) for k in range(c)], ey)
            face = face + jnp.where(join_low_x, low, jnp.where(join_high_x, high, 0.0))
            send_y[r, side] = face
            send_e[r, 4 + 2 * side] = face[0:1]
            send_e[r, 5 + 2 * side] = face[7:8]

        def pack(side, b):
            shift = 16 * b - 124 * side
            return by_slot([turn(rows[b][k], shift + 4 * k, 1) for k in range(c)], ex)

        packed = [[pack(side, b) if b in (0, 7) else None for b in range(8)] for side in range(2)]
        for side in range(2):
            corner = jnp.where(pack_b < 4, packed[side][0], packed[side][7])
            send_e[r, 8 + 2 * side] = corner[0:1]
            send_e[r, 9 + 2 * side] = corner[7:8]
        start(r, c, far)
        v = list(v)
        for side in range(2):
            v[7 * side] = join_x(join_y(v[7 * side]))
            send_z[r, side, pl.ds(0, c)] = v[7 * side]
        for side in range(2):
            face = merge(
                [packed[side][b] if b in (0, 7) else pack(side, b) for b in range(8)], pack_b
            )
            low, high = turn(face, 17, 1), turn(face, -17, 1)
            face = face + jnp.where(pack_low_y, low, jnp.where(pack_high_y, high, 0.0))
            send_x[r, side] = face
            send_e[r, 2 * side] = face[0:1]
            send_e[r, 2 * side + 1] = face[7:8]
        start(r, c, near_edges + near)
        for t in range(1, 7):
            v[t] = join_x(join_y(v[t]))
        if hook is not None:
            hook()
        finish(r, c, near)
        faces = []
        for dx in (-1, 1):
            low = turn(recv_xy[r, column(dx, -1)], 13, 1)
            high = turn(recv_xy[r, column(dx, 1)], -13, 1)
            faces.append(
                recv_xy[r, column(dx, 0)]
                + jnp.where(edge_low_y, low, jnp.where(edge_high_y, high, 0.0))
            )
        for side in range(2):
            v[7 * side] = v[7 * side] + recv_z[r, side, :c]
        finish(r, c, far + near_edges)
        faces = [faces[i] + edge_rows(r, 2 * i - 1, 0) for i in range(2)]
        sides = [recv_xy[r, column(0, dy)] + edge_rows(r, 0, dy) for dy in (-1, 1)]
        corners = [[edge_rows(r, dx, dy) for dx in (-1, 1)] for dy in (-1, 1)]
        for b in (0, 7, 1, 2, 3, 4, 5, 6):
            for k in range(c):
                low = turn(faces[0], -16 * b - 4 * k, 1)
                high = turn(faces[1], 124 - 16 * b - 4 * k, 1)
                part = jnp.where(lane8 < 4, low, jnp.where(lane8 >= 124, high, 0.0))
                if b in (0, 7):
                    side = b // 7
                    slot = 3 * side
                    part = part + jnp.where(ey == slot, turn(sides[side], slot - k, 1), 0.0)
                    begin = slot - 4 * k - 115 * (1 - side)
                    low = turn(corners[side][0], begin, 1)
                    high = turn(corners[side][1], begin + 124, 1)
                    part = part + jnp.where(
                        lane8 == slot, low, jnp.where(lane8 == 124 + slot, high, 0.0)
                    )
                work_c[k, pl.ds(b, 8, stride=8), :] = part
        corrections = planes_of(work_c, c)
        return [v[t] + corrections[t] for t in range(8)]

    def advect(v):
        dx = along_x(v, fwd_ref)
        dy = along_y(v, deriv, -1)
        dz = along_index(deriv, -1, v)
        return [
            velocity[t][0:1] * dx[t] + velocity[t][1:2] * dy[t] + velocity[t][2:3] * dz[t]
            for t in range(8)
        ]

    loads[3].wait()
    first = advect(velocity)
    diag, quad, mobile = [], [], []

    def diagonal():
        clear()
        for load in loads[4:]:
            load.wait()
        plane = plane_ref[...].reshape(1, 8, 128)
        quad.extend(plane * float(weights[t]) for t in range(8))
        mobile.extend(quad[t] * planes[t][3:4] for t in range(8))
        square_x = along_x(mobile, sqr_ref)
        square_y = along_y(mobile, squared_t, 1)
        square_z = along_index(squared_t, 1, mobile)
        diag.extend(
            mass_shift * quad[t] + square_x[t] + square_y[t] + square_z[t] for t in range(8)
        )

    pl.semaphore_wait(barrier, others)
    first = assemble(first, 0, diagonal)
    k1 = [first[t] * share[t] for t in range(8)]
    total_rate = k1
    v = [velocity[t] - (0.5 * time_step) * k1[t] for t in range(8)]
    for r, step, weight in ((1, 0.5, 2.0), (2, 1.0, 2.0), (3, 0.0, 1.0)):
        g = advect(v)
        if r == 1:
            g = assemble([jnp.concatenate([g[t], diag[t]], axis=0) for t in range(8)], r)
            inverse_jacobi = [1.0 / g[t][3:4] for t in range(8)]
            g = [g[t][0:3] for t in range(8)]
        else:
            g = assemble(g, r)
        g = [g[t] * share[t] for t in range(8)]
        total_rate = [total_rate[t] + weight * g[t] for t in range(8)]
        if step:
            v = [velocity[t] - (step * time_step) * g[t] for t in range(8)]
    advected = [velocity[t] - (time_step / 6.0) * total_rate[t] for t in range(8)]

    div_x = along_x([advected[t][0:1] for t in range(8)], fwd_ref)
    div_y = along_y([advected[t][1:2] for t in range(8)], deriv, -1)
    div_z = along_index(deriv, -1, [advected[t][2:3] for t in range(8)])
    div = [div_x[t] + div_y[t] + div_z[t] for t in range(8)]

    def put_advected():
        parts = [[advected[t][i] for t in range(8)] for i in range(3)]
        adv_ref[0], adv_ref[1] = give(parts[0], parts[1])
        adv_ref[2], _ = give(parts[2], parts[2])

    total_div = assemble(div, 4, put_advected)
    r0 = [total_div[t] * (quad[t] * (-1.0 / time_step)) for t in range(8)]

    def slopes(v):
        return along_x(v, fwd_ref), along_y(v, deriv, -1), along_index(deriv, -1, v)

    def flux(slope):
        return [[mobile[t] * part[t] for t in range(8)] for part in slope]

    def local(v, flow):
        bx = along_x(flow[0], bwd_ref)
        by = along_y(flow[1], deriv_t, -1)
        bz = along_index(deriv_t, -1, flow[2])
        return [(mass_shift * quad[t]) * v[t] + bx[t] + by[t] + bz[t] for t in range(8)]

    def energy_row(v, slope, flow):
        acc = None
        for t in range(8):
            term = (mass_shift * quad[t]) * (v[t] * v[t])
            for i in range(3):
                term = term + flow[i][t] * slope[i][t]
            acc = term if acc is None else acc + term
        return jnp.sum(acc[0], axis=0, keepdims=True)

    def dot_row(a, b, scale=None):
        acc = None
        for t in range(8):
            term = a[t] * b[t]
            if scale is not None:
                term = term * scale[t]
            acc = term if acc is None else acc + term
        return jnp.sum(acc[0], axis=0, keepdims=True)

    given = {}

    def give_first():
        given["r0"], given["z0"] = give(r0, z0)

    def give_second():
        given["s"], given["w"] = give(s, w)

    z0 = [r0[t] * inverse_jacobi[t] for t in range(8)]
    slope = slopes(z0)
    flow = flux(slope)
    lz = local(z0, flow)
    rho_row = dot_row(r0, z0, share)
    gamma_row = energy_row(z0, slope, flow)
    s = assemble(lz, 5, give_first)
    w = [s[t] * inverse_jacobi[t] for t in range(8)]
    delta_row = dot_row(s, w, share)
    slope = slopes(w)
    flow = flux(slope)
    eps_row = energy_row(w, slope, flow)
    partial = jnp.concatenate(
        [rho_row, gamma_row, delta_row, eps_row, jnp.zeros((4, 128), f32)], axis=0
    )
    partial = jnp.sum(partial, axis=1, keepdims=True)
    own = jnp.sum(jnp.where(sub8 == lane8, partial, 0.0), axis=0, keepdims=True)
    sums[...] = own

    def share_sums(device, index):
        pltpu.make_async_remote_copy(
            src_ref=sums,
            dst_ref=sums_in.at[index],
            send_sem=sum_send,
            recv_sem=sum_recv,
            device_id=device,
            device_id_type=MESH,
        ).start()

    each_other(share_sums)
    t_vec = assemble(local(w, flow), 6, give_second)
    third, _ = give(t_vec, t_vec)
    arrived = pltpu.make_async_remote_copy(
        src_ref=sums_in,
        dst_ref=sums_in,
        send_sem=sum_send,
        recv_sem=sum_recv,
        device_id=tuple(lax.rem(me[i] + 1, counts[i]) for i in range(3)),
        device_id_type=MESH,
    )
    sent()
    arrived.wait_send()
    arrived.wait_recv()
    joined = own + jnp.sum(sums_in[...], axis=0)
    four = jnp.sum(jnp.where(sub8 == lane8, joined, 0.0), axis=1, keepdims=True)
    rho, gamma, delta, eps = (four[i : i + 1] for i in range(4))
    alpha0 = rho / gamma
    rho1 = rho - 2.0 * alpha0 * gamma + alpha0 * alpha0 * delta
    beta = rho1 / rho
    cross = gamma - alpha0 * delta
    curve = gamma - 2.0 * alpha0 * delta + alpha0 * alpha0 * eps
    curve = curve + 2.0 * beta * cross + beta * beta * gamma
    alpha1 = rho1 / curve
    along = alpha0 + alpha1 * (1.0 + beta)
    side_step = alpha0 * alpha1

    pre_ref[...] = along * given["z0"] - side_step * given["w"]
    res_ref[...] = given["r0"] - along * given["s"] + side_step * third


def finish_kernel(adv_ref, pre_ref, res_ref, adv_out, pre_out, res_out):
    adv_out[...] = adv_ref[...]
    pre_out[...] = pre_ref[...]
    res_out[...] = res_ref[...]


def per_device(counts, velocity, inv_density, element_place):
    f32 = jnp.float32
    plane, forward, backward, square = constants()
    elements = element_place.shape[0]
    points = inv_density.shape[0]
    vmem = pl.BlockSpec(memory_space=pltpu.VMEM)
    faces = pltpu.VMEM((ROUNDS, 2, 8, 128), f32)
    faces_z = pltpu.VMEM((ROUNDS, 2, 4, 8, 128), f32)
    work = pltpu.VMEM((4, 64, 128), f32)
    dma = pltpu.SemaphoreType.DMA
    others = counts[0] * counts[1] * counts[2] - 1
    shapes = (
        jax.ShapeDtypeStruct((3, elements, points), f32),
        jax.ShapeDtypeStruct((elements, points), f32),
        jax.ShapeDtypeStruct((elements, points), f32),
    )
    computed = pl.pallas_call(
        functools.partial(kernel, counts),
        out_shape=shapes,
        in_specs=[pl.BlockSpec(memory_space=pltpu.HBM)] * 7,
        out_specs=(vmem, vmem, vmem),
        scratch_shapes=[
            faces,
            faces,
            faces_z,
            pltpu.VMEM((ROUNDS, 12, 1, 128), f32),
            pltpu.VMEM((ROUNDS, 9, 8, 128), f32),
            faces_z,
            pltpu.VMEM((ROUNDS, 27, 1, 128), f32),
            work,
            work,
            work,
            work,
            pltpu.VMEM((1, 128), f32),
            pltpu.VMEM((others, 1, 128), f32),
            dma((27,)),
            dma((ROUNDS, 27)),
            dma,
            dma,
            pltpu.VMEM((3, elements, points), f32),
            pltpu.VMEM((elements, points), f32),
            pltpu.SMEM((elements,), jnp.int32),
            pltpu.VMEM(plane.shape, f32),
            pltpu.VMEM(forward.shape, jnp.bfloat16),
            pltpu.VMEM(backward.shape, jnp.bfloat16),
            pltpu.VMEM(square.shape, jnp.bfloat16),
            dma((7,)),
        ],
        compiler_params=pltpu.CompilerParams(
            collective_id=0, has_side_effects=True, vmem_limit_bytes=VMEM_LIMIT
        ),
    )(
        *(
            pltpu.with_memory_space_constraint(operand, pltpu.HBM)
            for operand in (
                velocity.transpose(0, 2, 1),
                inv_density.T,
                element_place,
                jnp.asarray(plane),
                jnp.asarray(forward),
                jnp.asarray(backward),
                jnp.asarray(square),
            )
        )
    )
    advected, pressure, residual = pl.pallas_call(
        finish_kernel,
        out_shape=shapes,
        in_specs=[vmem, vmem, vmem],
        out_specs=(vmem, vmem, vmem),
        compiler_params=pltpu.CompilerParams(vmem_limit_bytes=VMEM_LIMIT),
    )(*computed)
    return advected.transpose(0, 2, 1), pressure.T, residual.T


def solution(mesh):
    counts = tuple(mesh.shape[name] for name in AXES)
    placed = (P(None, None, AXES), P(None, AXES), P(AXES))
    return jax.shard_map(
        functools.partial(per_device, counts),
        mesh=mesh,
        in_specs=placed,
        out_specs=(P(None, None, AXES), P(None, AXES), P(None, AXES)),
        check_vma=False,
    )
```

```python
import functools

import jax
import jax.numpy as jnp
import numpy as np
from jax import lax
from jax.experimental import pallas as pl
from jax.experimental.pallas import tpu as pltpu
from jax.sharding import PartitionSpec as P

BX = 4
BY = 4
BZ = 1
MESH = pl.DeviceIdType.MESH
AXES = ("gx", "gy", "gz")
ROUNDS = 7
VMEM_LIMIT = 16 << 20

time_step = 0.03
mass_shift = 4.0
inner_nodes = (
    -0.8717401485096066,
    -0.5917001814331423,
    -0.2092992179024789,
    0.2092992179024789,
    0.5917001814331423,
    0.8717401485096066,
)


def legendre_seven(position):
    previous = 1.0
    current_value = position
    for degree_index in range(1, 7):
        following = (
            (2 * degree_index + 1) * position * current_value - degree_index * previous
        ) / (degree_index + 1)
        previous = current_value
        current_value = following
    return current_value


def tables():
    nodes = [-1.0] + list(inner_nodes) + [1.0]
    poly = [legendre_seven(node) for node in nodes]
    weights = np.array([2.0 / (56.0 * value * value) for value in poly])
    derivative = np.zeros((8, 8))
    for i in range(8):
        for j in range(8):
            if i != j:
                derivative[i, j] = poly[i] / (poly[j] * (nodes[i] - nodes[j]))
    derivative[0, 0] = -14.0
    derivative[7, 7] = 14.0
    return weights, derivative.astype(np.float32).astype(np.float64)


def split_stack(matrix):
    high = np.asarray(matrix, np.float32).astype(jnp.bfloat16)
    low = (np.asarray(matrix, np.float32) - high.astype(np.float32)).astype(jnp.bfloat16)
    return np.concatenate([high, high, low], axis=0)


LANE_NODES = (0, 2, 4, 6, 1, 3, 5, 7)


@functools.cache
def constants():
    weights, d = tables()
    nodes = list(LANE_NODES)
    eye16 = np.eye(16)

    def lanes(matrix):
        return split_stack(np.kron(matrix[np.ix_(nodes, nodes)], eye16))

    plane = np.outer(weights, np.repeat(weights[nodes], 16))
    return plane.astype(np.float32), lanes(d.T), lanes(d), lanes(d**2)


def along_index(matrix, sign, v):
    plus = [v[j] + v[7 - j] for j in range(4)]
    minus = [v[j] - v[7 - j] for j in range(4)]
    out = [None] * 8
    for i in range(4):
        even = odd = None
        for j in range(4):
            p = float(0.5 * (matrix[i, j] + matrix[i, 7 - j])) * plus[j]
            n = float(0.5 * (matrix[i, j] - matrix[i, 7 - j])) * minus[j]
            even = p if even is None else even + p
            odd = n if odd is None else odd + n
        out[i] = even + odd
        out[7 - i] = even - odd if sign > 0 else odd - even
    return out


def kernel(
    counts,
    vel_hbm,
    den_hbm,
    place_hbm,
    plane_hbm,
    fwd_hbm,
    bwd_hbm,
    sqr_hbm,
    adv_ref,
    pre_ref,
    res_ref,
    send_x,
    send_y,
    send_z,
    send_e,
    recv_xy,
    recv_z,
    recv_e,
    work_v,
    work_d,
    work_g,
    work_c,
    sums,
    sums_in,
    send_sem,
    recv_sem,
    sum_send,
    sum_recv,
    vel_ref,
    den_ref,
    place_ref,
    plane_ref,
    fwd_ref,
    bwd_ref,
    sqr_ref,
    load_sem,
):
    f32 = jnp.float32
    loads = [
        pltpu.make_async_copy(source_ref, target_ref, load_sem.at[index])
        for index, (source_ref, target_ref) in enumerate(
            (
                (place_hbm, place_ref),
                (vel_hbm, vel_ref),
                (den_hbm, den_ref),
                (fwd_hbm, fwd_ref),
                (plane_hbm, plane_ref),
                (sqr_hbm, sqr_ref),
                (bwd_hbm, bwd_ref),
            )
        )
    ]
    for load in loads:
        load.start()
    me = [lax.axis_index(name) for name in AXES]
    has = [(me[i] > 0, me[i] < counts[i] - 1) for i in range(3)]
    weights, deriv = tables()
    deriv_t, squared_t = deriv.T, deriv.T**2

    def each_other(act):
        for kx in range(counts[0]):
            for ky in range(counts[1]):
                base = (kx * counts[1] + ky) * counts[2]
                first = 0 if base else 1

                def one(kz, _):
                    steps = (kx, ky, kz)
                    device = tuple(lax.rem(me[i] + steps[i], counts[i]) for i in range(3))
                    act(device, base + kz - 1)
                    return 0

                if counts[2] <= 8:
                    for kz in range(first, counts[2]):
                        one(kz, 0)
                else:
                    lax.fori_loop(first, counts[2], one, 0)

    directions = [
        (dx, dy, dz)
        for dx in (-1, 0, 1)
        for dy in (-1, 0, 1)
        for dz in (-1, 0, 1)
        if (dx, dy, dz) != (0, 0, 0)
    ]

    def exists(d):
        flag = None
        for i in range(3):
            if d[i]:
                here = has[i][1 if d[i] > 0 else 0]
                flag = here if flag is None else jnp.logical_and(flag, here)
        return flag

    peers = {d: (exists(d), tuple(me[i] + d[i] for i in range(3))) for d in directions}
    far = [d for d in directions if d[1] and d[2]]
    far.sort(key=lambda d: abs(d[0]))
    up_down = [(0, 0, -1), (0, 0, 1)]
    cross = [d for d in directions if d[0] and d[2] and not d[1]]
    flat = [d for d in directions if not d[2]]
    flat.sort(key=lambda d: (-abs(d[1]), abs(d[0])))

    barrier = pltpu.get_barrier_semaphore()

    def greet(device, index):
        pl.semaphore_signal(barrier, inc=1, device_id=device, device_id_type=MESH)

    if max(counts) <= ROUNDS:
        for d in directions:

            @pl.when(peers[d][0])
            def _():
                greet(peers[d][1], 0)

        greeted = 1
        for i in range(3):
            low, high = has[i]
            greeted = greeted * (1 + low.astype(jnp.int32) + high.astype(jnp.int32))
        others = greeted - 1
    else:
        each_other(greet)
        others = counts[0] * counts[1] * counts[2] - 1

    sub8 = lax.broadcasted_iota(jnp.int32, (8, 128), 0)
    lane8 = lax.broadcasted_iota(jnp.int32, (8, 128), 1)
    ex, ey = (lane8 // 4) % 4, lane8 % 4
    low_x, high_x = lane8 < 16, lane8 >= 112
    join_low_x, join_high_x = low_x & (ex > 0), high_x & (ex < 3)
    join_low_y, join_high_y = (sub8 == 0) & (ey > 0), (sub8 == 7) & (ey < 3)
    pack_b = lane8 // 16
    pack_low_y, pack_high_y = (pack_b == 0) & (ey > 0), (pack_b == 7) & (ey < 3)
    origin = [(lane8 - 3 - (lane8 + 1) % 4) % 128, (lane8 + 3 - lane8 % 4) % 128]
    edge_join_low = [(o < 16) & ((o // 4) % 4 > 0) for o in origin]
    edge_join_high = [(o >= 112) & ((o // 4) % 4 < 3) for o in origin]
    far_y = ((sub8 == 0) & (ey == 0)) | ((sub8 == 7) & (ey == 3))
    far_low = (sub8 == 0) & ((lane8 == 0) | (lane8 == 124))
    far_high = (sub8 == 7) & ((lane8 == 3) | (lane8 == 127))
    far_corner = far_low | far_high
    edge_low_y, edge_high_y = (pack_b == 0) & (ey == 0), (pack_b == 7) & (ey == 3)

    def half(flag):
        return jnp.where(flag, 0.5, 1.0).astype(f32)

    total = [BX * counts[0], BY * counts[1], BZ * counts[2]]
    pos_x, pos_y = ex + me[0] * BX, ey + me[1] * BY
    share_xy = half((low_x & (pos_x > 0)) | (high_x & (pos_x < total[0] - 1)))
    share_xy = share_xy * half(
        ((sub8 == 0) & (pos_y > 0)) | ((sub8 == 7) & (pos_y < total[1] - 1))
    )
    share_xy = share_xy.reshape(1, 8, 128)
    share = [share_xy] * 8
    share[0] = share_xy * half(has[2][0])
    share[7] = share_xy * half(has[2][1])

    def turn(x, shift, axis):
        size = x.shape[axis]
        shift = shift % size
        return pltpu.roll(x, shift, axis) if shift else x

    def rows_of(ref, count):
        return [
            jnp.stack([ref[k, pl.ds(b, 8, stride=8), :] for k in range(count)])
            for b in range(8)
        ]

    def planes_of(ref, count):
        return [
            jnp.stack([ref[k, 8 * c : 8 * c + 8, :] for k in range(count)]) for c in range(8)
        ]

    def put_rows(ref, rows):
        for b in range(8):
            for k in range(rows[b].shape[0]):
                ref[k, pl.ds(b, 8, stride=8), :] = rows[b][k]

    def put_planes(ref, planes):
        for c in range(8):
            for k in range(planes[c].shape[0]):
                ref[k, 8 * c : 8 * c + 8, :] = planes[c][k]

    loads[0].wait()
    r16 = lax.broadcasted_iota(jnp.int32, (16, 16), 0)
    l16 = lax.broadcasted_iota(jnp.int32, (16, 16), 1)
    by_lane = jnp.zeros((16, 16), jnp.int32)
    by_row = jnp.zeros((16, 16), jnp.int32)
    for e in range(16):
        by_lane = jnp.where(l16 == e, place_ref[e], by_lane)
        by_row = jnp.where(r16 == e, place_ref[e], by_row)
    to_place = jnp.concatenate([(by_lane == r16).astype(f32)] * 3, axis=1)
    to_slot = jnp.concatenate([(by_row == l16).astype(f32)] * 3, axis=1)

    def order(matrix, block):
        high = block.astype(jnp.bfloat16).astype(f32)
        rest = block - high
        middle = rest.astype(jnp.bfloat16).astype(f32)
        parts = jnp.concatenate([high, middle, rest - middle], axis=0)
        return jnp.dot(
            matrix.astype(jnp.bfloat16),
            parts.astype(jnp.bfloat16),
            preferred_element_type=f32,
        )

    lane64 = lax.broadcasted_iota(jnp.int32, (64, 128), 1)

    def take(first, second):
        blocks = [
            order(to_place, field)[:, 128 * t : 128 * t + 128]
            for field in (first, second)
            for t in range(4)
        ]
        turned = jnp.concatenate(blocks, axis=0).T
        top, bottom = turned[:64], turned[64:]
        left = jnp.where(lane64 < 64, top, turn(bottom, 64, 1))
        right = jnp.where(lane64 < 64, turn(top, 64, 1), bottom)
        return left, right

    def give(first, second):
        for k, field in enumerate((first, second)):
            for c in range(8):
                work_d[k, 8 * c : 8 * c + 8, :] = field[c].reshape(8, 128)
        left, right = (
            jnp.concatenate(
                [work_d[k, pl.ds(b, 8, stride=8), :] for b in range(8)], axis=0
            )
            for k in range(2)
        )
        top = jnp.where(lane64 < 64, left, turn(right, 64, 1))
        bottom = jnp.where(lane64 < 64, turn(left, 64, 1), right)
        turned = jnp.concatenate([top, bottom], axis=0).T
        return [
            order(
                to_slot,
                jnp.concatenate(
                    [turned[64 * k + 16 * t : 64 * k + 16 * t + 16] for t in range(4)], axis=1
                ),
            )
            for k in range(2)
        ]

    loads[1].wait()
    loads[2].wait()
    taken = [*take(vel_ref[0], vel_ref[1]), *take(vel_ref[2], den_ref[...])]
    put_rows(
        work_v, [jnp.stack([f[8 * b : 8 * b + 8] for f in taken]) for b in range(8)]
    )
    planes = planes_of(work_v, 4)
    velocity = [planes[c][0:3] for c in range(8)]

    def split(x):
        high = x.astype(jnp.bfloat16)
        low = (x - high.astype(f32)).astype(jnp.bfloat16)
        return jnp.concatenate([high, low, high], axis=1)

    def along_y(v, matrix, sign):
        c = v[0].shape[0]
        put_planes(work_v, v)
        put_rows(work_d, along_index(matrix, sign, rows_of(work_v, c)))
        return planes_of(work_d, c)

    def code(d):
        return (d[0] + 1) * 9 + (d[1] + 1) * 3 + d[2] + 1

    def side_of(step):
        return 1 if step > 0 else 0

    def column(dx, dy):
        return 3 * (dx + 1) + dy + 1

    def edge_slot(d):
        if d[0] and d[1]:
            return 8 + 4 * side_of(d[0]) + 2 * side_of(d[1]) + side_of(d[2])
        return (0 if d[0] else 4) + 2 * side_of(d[0] or d[1]) + side_of(d[2])

    def source(r, d, c):
        if not d[0] and not d[1]:
            return send_z.at[r, side_of(d[2]), pl.ds(0, c)]
        if d[2]:
            return send_e.at[r, edge_slot(d)]
        return (send_x if d[0] else send_y).at[r, side_of(d[0] if d[0] else d[1])]

    def target(r, d, c):
        if not d[0] and not d[1]:
            return recv_z.at[r, side_of(d[2]), pl.ds(0, c)]
        if d[2]:
            return recv_e.at[r, code(d)]
        return recv_xy.at[r, column(d[0], d[1])]

    def copy(r, d, c, incoming):
        back = d if incoming else tuple(-i for i in d)
        return pltpu.make_async_remote_copy(
            src_ref=source(r, d, c),
            dst_ref=target(r, back, c),
            send_sem=send_sem.at[code(d)],
            recv_sem=recv_sem.at[r, code(back)],
            device_id=peers[d][1],
            device_id_type=MESH,
        )

    def start(r, c, group):
        for d in group:

            @pl.when(peers[d][0])
            def _():
                copy(r, d, c, False).start()

    def finish(r, c, group):
        for d in group[::-1]:

            @pl.when(peers[d][0])
            def _():
                copy(r, d, c, True).wait_recv()

    def sent():
        for d in directions:
            if not d[0] and not d[1]:
                ref = recv_z.at[pl.ds(0, 2)]
            elif d[2]:
                ref = recv_e.at[:, 0]
            else:
                ref = recv_xy.at[:, 0]

            @pl.when(peers[d][0])
            def _():
                pltpu.make_async_remote_copy(
                    src_ref=ref,
                    dst_ref=ref,
                    send_sem=send_sem.at[code(d)],
                    recv_sem=recv_sem.at[0, code(d)],
                    device_id=peers[d][1],
                    device_id_type=MESH,
                ).wait_send()

    def clear():
        for d in directions:

            @pl.when(jnp.logical_not(peers[d][0]))
            def _():
                for r in range(ROUNDS):
                    if not d[0] and not d[1]:
                        recv_z[r, side_of(d[2])] = jnp.zeros((4, 8, 128), f32)
                    elif d[2]:
                        recv_e[r, code(d)] = jnp.zeros((1, 128), f32)
                    else:
                        recv_xy[r, column(d[0], d[1])] = jnp.zeros((8, 128), f32)

    def join_x(v):
        low, high = turn(v, 20, 2), turn(v, -20, 2)
        return v + jnp.where(join_low_x, low, jnp.where(join_high_x, high, 0.0))

    def join_y(v):
        low, high = turn(turn(v, 1, 1), 1, 2), turn(turn(v, -1, 1), -1, 2)
        return v + jnp.where(join_low_y, low, jnp.where(join_high_y, high, 0.0))

    def join_xy(v):
        up, down = turn(v, 1, 1), turn(v, -1, 1)
        low, high = turn(v, 20, 2), turn(v, -20, 2)
        out = v + jnp.where(join_low_x, low, jnp.where(join_high_x, high, 0.0))
        for face, step, mask in ((up, 1, join_low_y), (down, -1, join_high_y)):
            part = turn(face, step, 2)
            low, high = turn(face, step + 20, 2), turn(face, step - 20, 2)
            part = part + jnp.where(join_low_x, low, jnp.where(join_high_x, high, 0.0))
            out = out + jnp.where(mask, part, 0.0)
        return out

    def merge(parts, index, bit=1):
        while len(parts) > 1:
            parts = [
                jnp.where((index & bit) == 0, parts[i], parts[i + 1])
                for i in range(0, len(parts), 2)
            ]
            bit *= 2
        return parts[0]

    def by_slot(parts, slot):
        acc = parts[0]
        for k in range(1, len(parts)):
            acc = jnp.where(slot == k, parts[k], acc)
        return acc

    def edge_rows(r, dx, dy):
        low, high = recv_e[r, code((dx, dy, -1))], recv_e[r, code((dx, dy, 1))]
        return jnp.where(sub8 == 0, low, jnp.where(sub8 == 7, high, 0.0))

    def send_far(r, dz, v):
        c = v.shape[0]
        for side, dy in enumerate((-1, 1)):
            shift = -3 * dy if side else 3
            slot = (ey + 1 - side) % 4
            face = by_slot([turn(v[k], k + shift, 1) for k in range(c)], slot)
            low = by_slot([turn(v[k], k + shift + 20, 1) for k in range(c)], slot)
            high = by_slot([turn(v[k], k + shift - 20, 1) for k in range(c)], slot)
            face = face + jnp.where(
                edge_join_low[side], low, jnp.where(edge_join_high[side], high, 0.0)
            )
            row = 7 * side
            send_e[r, edge_slot((0, dy, dz))] = face[row : row + 1]
            for dx in (-1, 1):
                shift_x = -124 * dx - 3 * dy
                corner = by_slot(
                    [turn(v[k], shift_x + 16 * k, 1) for k in range(c)],
                    ((lane8 + 4) // 16) % 8,
                )
                send_e[r, edge_slot((dx, dy, dz))] = corner[row : row + 1]

    def take_far(r, dz, c):
        face = jnp.where(
            sub8 == 0,
            recv_e[r, code((0, -1, dz))],
            jnp.where(sub8 == 7, recv_e[r, code((0, 1, dz))], 0.0),
        )
        inner = lane8 % 16 < 4
        rows = [
            jnp.where(inner, recv_e[r, code((-1, dy, dz))], recv_e[r, code((1, dy, dz))])
            for dy in (-1, 1)
        ]
        corner = jnp.where(sub8 == 0, rows[0], jnp.where(sub8 == 7, rows[1], 0.0))
        return jnp.stack(
            [
                jnp.where(far_y, turn(face, -k, 1), 0.0)
                + jnp.where(far_corner, turn(corner, -16 * k, 1), 0.0)
                for k in range(c)
            ]
        )

    def assemble(v, r, hook=None):
        for side in range(2):
            send_far(r, 2 * side - 1, v[7 * side])
        c = v[0].shape[0]
        for side in range(2):
            send_z[r, side, pl.ds(0, c)] = v[7 * side]
        v = list(v)
        put_planes(work_g, v)
        rows = [
            [work_g[k, pl.ds(b, 8, stride=8), :] for k in range(c)] for b in range(8)
        ]
        for side in range(2):
            own = rows[7 * side]
            face = by_slot([turn(own[k], k - 3 * side, 1) for k in range(c)], ey)
            low = by_slot([turn(own[k], k - 3 * side + 20, 1) for k in range(c)], ey)
            high = by_slot([turn(own[k], k - 3 * side - 20, 1) for k in range(c)], ey)
            send_y[r, side] = face + jnp.where(
                join_low_x, low, jnp.where(join_high_x, high, 0.0)
            )
        start(r, c, far + flat[:2] + up_down)
        for side in range(2):
            packed = []
            for b in range(8):
                shift = 16 * b - 124 * side
                packed.append(by_slot([turn(rows[b][k], shift + 4 * k, 1) for k in range(c)], ex))
            face = merge(packed, pack_b)
            shift = -124 * side
            low = by_slot([turn(rows[7][k], shift + 4 * k + 1, 1) for k in range(c)], ex)
            shift += 112
            high = by_slot([turn(rows[0][k], shift + 4 * k - 1, 1) for k in range(c)], ex)
            face = face + jnp.where(pack_low_y, low, jnp.where(pack_high_y, high, 0.0))
            send_x[r, side] = face
            send_e[r, 2 * side] = face[0:1]
            send_e[r, 2 * side + 1] = face[7:8]
        start(r, c, cross + flat[2:])
        for t in range(1, 7):
            v[t] = join_x(join_y(v[t]))
        if hook is not None:
            hook()
        finish(r, c, flat + up_down + cross)
        faces = [recv_xy[r, column(dx, 0)] + edge_rows(r, dx, 0) for dx in (-1, 1)]
        for side in range(2):
            v[7 * side] = join_xy(v[7 * side] + recv_z[r, side, :c])
        for b in range(8):
            for k in range(c):
                low = turn(faces[0], -16 * b - 4 * k, 1)
                high = turn(faces[1], 124 - 16 * b - 4 * k, 1)
                part = jnp.where(lane8 < 4, low, jnp.where(lane8 >= 124, high, 0.0))
                if b in (0, 7):
                    side = b // 7
                    dy, slot = 2 * side - 1, 3 * side
                    face = turn(recv_xy[r, column(0, dy)], slot - k, 1)
                    part = part + jnp.where(ey == slot, face, 0.0)
                    begin = slot - 4 * k - 115 * (1 - side)
                    low = turn(recv_xy[r, column(-1, dy)], begin, 1)
                    high = turn(recv_xy[r, column(1, dy)], begin + 124, 1)
                    part = part + jnp.where(
                        lane8 == slot, low, jnp.where(lane8 == 124 + slot, high, 0.0)
                    )
                work_c[k, pl.ds(b, 8, stride=8), :] = part
        corrections = planes_of(work_c, c)
        v = [v[t] + corrections[t] for t in range(8)]
        finish(r, c, far)
        for side in range(2):
            v[7 * side] = v[7 * side] + take_far(r, 2 * side - 1, c)
        return v

    def along_x(v, w_ref):
        c = v[0].shape[0]
        x = jnp.concatenate([v[t].reshape(c * 8, 128) for t in range(8)], axis=0)
        y = jnp.dot(split(x), w_ref[...], preferred_element_type=f32)
        return [y[t * c * 8 : (t + 1) * c * 8].reshape(c, 8, 128) for t in range(8)]

    def advect(v):
        dx = along_x(v, fwd_ref)
        dy = along_y(v, deriv, -1)
        dz = along_index(deriv, -1, v)
        return [
            velocity[t][0:1] * dx[t] + velocity[t][1:2] * dy[t] + velocity[t][2:3] * dz[t]
            for t in range(8)
        ]

    loads[3].wait()
    diag, quad, mobile = [], [], []

    def diagonal():
        clear()
        for load in loads[4:]:
            load.wait()
        plane = plane_ref[...].reshape(1, 8, 128)
        quad.extend(plane * float(weights[t]) for t in range(8))
        mobile.extend(quad[t] * planes[t][3:4] for t in range(8))
        square_x = along_x(mobile, sqr_ref)
        square_y = along_y(mobile, squared_t, 1)
        square_z = along_index(squared_t, 1, mobile)
        diag.extend(
            mass_shift * quad[t] + square_x[t] + square_y[t] + square_z[t] for t in range(8)
        )

    rate = advect(velocity)
    pl.semaphore_wait(barrier, others)
    total_rate = None
    for r, step, weight in ((0, 0.5, 1.0), (1, 0.5, 2.0), (2, 1.0, 2.0), (3, 0.0, 1.0)):
        if r == 1:
            rate = [jnp.concatenate([rate[t], diag[t]], axis=0) for t in range(8)]
        g = assemble(rate, r, None if r else diagonal)
        if r == 1:
            inverse_jacobi = [1.0 / g[t][3:4] for t in range(8)]
        g = [g[t][0:3] * share[t] for t in range(8)]
        total_rate = [weight * g[t] + (total_rate[t] if r else 0.0) for t in range(8)]
        if step:
            rate = advect([velocity[t] - (step * time_step) * g[t] for t in range(8)])
    advected = [velocity[t] - (time_step / 6.0) * total_rate[t] for t in range(8)]
    div_x = along_x([advected[t][0:1] for t in range(8)], fwd_ref)
    div_y = along_y([advected[t][1:2] for t in range(8)], deriv, -1)
    div_z = along_index(deriv, -1, [advected[t][2:3] for t in range(8)])
    div = [div_x[t] + div_y[t] + div_z[t] for t in range(8)]

    def put_advected():
        parts = [[advected[t][i] for t in range(8)] for i in range(3)]
        adv_ref[0], adv_ref[1] = give(parts[0], parts[1])
        adv_ref[2], _ = give(parts[2], parts[2])

    total_div = assemble(div, 4, put_advected)
    r0 = [total_div[t] * (quad[t] * (-1.0 / time_step)) for t in range(8)]

    def slopes(v):
        return along_x(v, fwd_ref), along_y(v, deriv, -1), along_index(deriv, -1, v)

    def flux(slope):
        return [[mobile[t] * part[t] for t in range(8)] for part in slope]

    def local(v, flow):
        bx = along_x(flow[0], bwd_ref)
        by = along_y(flow[1], deriv_t, -1)
        bz = along_index(deriv_t, -1, flow[2])
        return [(mass_shift * quad[t]) * v[t] + bx[t] + by[t] + bz[t] for t in range(8)]

    def energy_row(v, slope, flow):
        acc = None
        for t in range(8):
            term = (mass_shift * quad[t]) * (v[t] * v[t])
            for i in range(3):
                term = term + flow[i][t] * slope[i][t]
            acc = term if acc is None else acc + term
        return jnp.sum(acc[0], axis=0, keepdims=True)

    def dot_row(a, b, scale=None):
        acc = None
        for t in range(8):
            term = a[t] * b[t]
            if scale is not None:
                term = term * scale[t]
            acc = term if acc is None else acc + term
        return jnp.sum(acc[0], axis=0, keepdims=True)

    given = {}

    def give_first():
        given["r0"], given["z0"] = give(r0, z0)

    def give_second():
        given["s"], given["w"] = give(s, w)

    z0 = [r0[t] * inverse_jacobi[t] for t in range(8)]
    slope = slopes(z0)
    flow = flux(slope)
    rho_row = dot_row(r0, z0, share)
    gamma_row = energy_row(z0, slope, flow)

    s = assemble(local(z0, flow), 5, give_first)
    w = [s[t] * inverse_jacobi[t] for t in range(8)]
    delta_row = dot_row(s, w, share)
    slope = slopes(w)
    flow = flux(slope)
    eps_row = energy_row(w, slope, flow)
    partial = jnp.concatenate(
        [rho_row, gamma_row, delta_row, eps_row, jnp.zeros((4, 128), f32)], axis=0
    )
    partial = jnp.sum(partial, axis=1, keepdims=True)
    own = jnp.sum(jnp.where(sub8 == lane8, partial, 0.0), axis=0, keepdims=True)
    sums[...] = own

    def share_sums(device, index):
        pltpu.make_async_remote_copy(
            src_ref=sums,
            dst_ref=sums_in.at[index],
            send_sem=sum_send,
            recv_sem=sum_recv,
            device_id=device,
            device_id_type=MESH,
        ).start()

    each_other(share_sums)
    t_vec = assemble(local(w, flow), 6, give_second)
    third, _ = give(t_vec, t_vec)
    arrived = pltpu.make_async_remote_copy(
        src_ref=sums_in,
        dst_ref=sums_in,
        send_sem=sum_send,
        recv_sem=sum_recv,
        device_id=tuple(lax.rem(me[i] + 1, counts[i]) for i in range(3)),
        device_id_type=MESH,
    )
    sent()
    arrived.wait_send()
    arrived.wait_recv()
    joined = own + jnp.sum(sums_in[...], axis=0)
    four = jnp.sum(jnp.where(sub8 == lane8, joined, 0.0), axis=1, keepdims=True)
    rho, gamma, delta, eps = (four[i : i + 1] for i in range(4))
    alpha0 = rho / gamma
    rho1 = rho - 2.0 * alpha0 * gamma + alpha0 * alpha0 * delta
    beta = rho1 / rho
    cross = gamma - alpha0 * delta
    curve = gamma - 2.0 * alpha0 * delta + alpha0 * alpha0 * eps
    curve = curve + 2.0 * beta * cross + beta * beta * gamma
    alpha1 = rho1 / curve
    along = alpha0 + alpha1 * (1.0 + beta)
    side_step = alpha0 * alpha1

    pre_ref[...] = along * given["z0"] - side_step * given["w"]
    res_ref[...] = given["r0"] - along * given["s"] + side_step * third


def finish_kernel(adv_ref, pre_ref, res_ref, adv_out, pre_out, res_out):
    adv_out[...] = adv_ref[...]
    pre_out[...] = pre_ref[...]
    res_out[...] = res_ref[...]


def per_device(counts, velocity, inv_density, element_place):
    f32 = jnp.float32
    plane, forward, backward, square = constants()
    elements = element_place.shape[0]
    points = inv_density.shape[0]
    vmem = pl.BlockSpec(memory_space=pltpu.VMEM)
    faces = pltpu.VMEM((ROUNDS, 2, 8, 128), f32)
    faces_z = pltpu.VMEM((ROUNDS, 2, 4, 8, 128), f32)
    work = pltpu.VMEM((4, 64, 128), f32)
    dma = pltpu.SemaphoreType.DMA
    others = counts[0] * counts[1] * counts[2] - 1
    shapes = (
        jax.ShapeDtypeStruct((3, elements, points), f32),
        jax.ShapeDtypeStruct((elements, points), f32),
        jax.ShapeDtypeStruct((elements, points), f32),
    )
    computed = pl.pallas_call(
        functools.partial(kernel, counts),
        out_shape=shapes,
        in_specs=[pl.BlockSpec(memory_space=pltpu.HBM)] * 7,
        out_specs=(vmem, vmem, vmem),
        scratch_shapes=[
            faces,
            faces,
            faces_z,
            pltpu.VMEM((ROUNDS, 16, 1, 128), f32),
            pltpu.VMEM((ROUNDS, 9, 8, 128), f32),
            faces_z,
            pltpu.VMEM((ROUNDS, 27, 1, 128), f32),
            work,
            work,
            work,
            work,
            pltpu.VMEM((1, 128), f32),
            pltpu.VMEM((others, 1, 128), f32),
            dma((27,)),
            dma((ROUNDS, 27)),
            dma,
            dma,
            pltpu.VMEM((3, elements, points), f32),
            pltpu.VMEM((elements, points), f32),
            pltpu.SMEM((elements,), jnp.int32),
            pltpu.VMEM(plane.shape, f32),
            pltpu.VMEM(forward.shape, jnp.bfloat16),
            pltpu.VMEM(backward.shape, jnp.bfloat16),
            pltpu.VMEM(square.shape, jnp.bfloat16),
            dma((7,)),
        ],
        compiler_params=pltpu.CompilerParams(
            collective_id=0, has_side_effects=True, vmem_limit_bytes=VMEM_LIMIT
        ),
    )(
        *(
            pltpu.with_memory_space_constraint(operand, pltpu.HBM)
            for operand in (
                velocity.transpose(0, 2, 1),
                inv_density.T,
                element_place,
                jnp.asarray(plane),
                jnp.asarray(forward),
                jnp.asarray(backward),
                jnp.asarray(square),
            )
        )
    )
    advected, pressure, residual = pl.pallas_call(
        finish_kernel,
        out_shape=shapes,
        in_specs=[vmem, vmem, vmem],
        out_specs=(vmem, vmem, vmem),
        compiler_params=pltpu.CompilerParams(vmem_limit_bytes=VMEM_LIMIT),
    )(*computed)
    return advected.transpose(0, 2, 1), pressure.T, residual.T


def solution(mesh):
    counts = tuple(mesh.shape[name] for name in AXES)
    placed = (P(None, None, AXES), P(None, AXES), P(AXES))
    return jax.shard_map(
        functools.partial(per_device, counts),
        mesh=mesh,
        in_specs=placed,
        out_specs=(P(None, None, AXES), P(None, AXES), P(None, AXES)),
        check_vma=False,
    )
```

```python
import functools

import jax
import jax.numpy as jnp
import numpy as np
from jax import lax
from jax.experimental import pallas as pl
from jax.experimental.pallas import tpu as pltpu
from jax.sharding import PartitionSpec as P

BX = 4
BY = 4
BZ = 1
MESH = pl.DeviceIdType.MESH
AXES = ("gx", "gy", "gz")
ROUNDS = 7
VMEM_LIMIT = 16 << 20

time_step = 0.03
mass_shift = 4.0
inner_nodes = (
    -0.8717401485096066,
    -0.5917001814331423,
    -0.2092992179024789,
    0.2092992179024789,
    0.5917001814331423,
    0.8717401485096066,
)


def legendre_seven(position):
    previous = 1.0
    current_value = position
    for degree_index in range(1, 7):
        following = (
            (2 * degree_index + 1) * position * current_value - degree_index * previous
        ) / (degree_index + 1)
        previous = current_value
        current_value = following
    return current_value


def tables():
    nodes = [-1.0] + list(inner_nodes) + [1.0]
    poly = [legendre_seven(node) for node in nodes]
    weights = np.array([2.0 / (56.0 * value * value) for value in poly])
    derivative = np.zeros((8, 8))
    for i in range(8):
        for j in range(8):
            if i != j:
                derivative[i, j] = poly[i] / (poly[j] * (nodes[i] - nodes[j]))
    derivative[0, 0] = -14.0
    derivative[7, 7] = 14.0
    return weights, derivative.astype(np.float32).astype(np.float64)


def split_stack(matrix):
    high = np.asarray(matrix, np.float32).astype(jnp.bfloat16)
    low = (np.asarray(matrix, np.float32) - high.astype(np.float32)).astype(jnp.bfloat16)
    return np.concatenate([high, high, low], axis=0)


LANE_NODES = (0, 2, 4, 6, 1, 3, 5, 7)


@functools.cache
def constants():
    weights, d = tables()
    nodes = list(LANE_NODES)
    eye16 = np.eye(16)

    def lanes(matrix):
        return split_stack(np.kron(matrix[np.ix_(nodes, nodes)], eye16))

    plane = np.outer(weights, np.repeat(weights[nodes], 16))
    return plane.astype(np.float32), lanes(d.T), lanes(d), lanes(d**2)


def along_index(matrix, sign, v):
    plus = [v[j] + v[7 - j] for j in range(4)]
    minus = [v[j] - v[7 - j] for j in range(4)]
    out = [None] * 8
    for i in range(4):
        even = odd = None
        for j in range(4):
            p = float(0.5 * (matrix[i, j] + matrix[i, 7 - j])) * plus[j]
            n = float(0.5 * (matrix[i, j] - matrix[i, 7 - j])) * minus[j]
            even = p if even is None else even + p
            odd = n if odd is None else odd + n
        out[i] = even + odd
        out[7 - i] = even - odd if sign > 0 else odd - even
    return out


def kernel(
    counts,
    vel_hbm,
    den_hbm,
    place_hbm,
    plane_hbm,
    fwd_hbm,
    bwd_hbm,
    sqr_hbm,
    adv_ref,
    pre_ref,
    res_ref,
    send_x,
    send_y,
    send_z,
    send_e,
    recv_xy,
    recv_z,
    recv_e,
    work_v,
    work_d,
    work_g,
    work_c,
    sums,
    sums_in,
    send_sem,
    recv_sem,
    sum_send,
    sum_recv,
    vel_ref,
    den_ref,
    place_ref,
    plane_ref,
    fwd_ref,
    bwd_ref,
    sqr_ref,
    load_sem,
):
    f32 = jnp.float32
    loads = [
        pltpu.make_async_copy(source_ref, target_ref, load_sem.at[index])
        for index, (source_ref, target_ref) in enumerate(
            (
                (place_hbm, place_ref),
                (vel_hbm, vel_ref),
                (den_hbm, den_ref),
                (fwd_hbm, fwd_ref),
                (plane_hbm, plane_ref),
                (sqr_hbm, sqr_ref),
                (bwd_hbm, bwd_ref),
            )
        )
    ]
    for load in loads[:2]:
        load.start()
    me = [lax.axis_index(name) for name in AXES]
    has = [(me[i] > 0, me[i] < counts[i] - 1) for i in range(3)]
    weights, deriv = tables()
    deriv_t, squared_t = deriv.T, deriv.T**2

    def each_other(act):
        for kx in range(counts[0]):
            for ky in range(counts[1]):
                base = (kx * counts[1] + ky) * counts[2]
                first = 0 if base else 1

                def one(kz, _):
                    steps = (kx, ky, kz)
                    device = tuple(lax.rem(me[i] + steps[i], counts[i]) for i in range(3))
                    act(device, base + kz - 1)
                    return 0

                if counts[2] <= 8:
                    for kz in range(first, counts[2]):
                        one(kz, 0)
                else:
                    lax.fori_loop(first, counts[2], one, 0)

    directions = [
        (dx, dy, dz)
        for dx in (-1, 0, 1)
        for dy in (-1, 0, 1)
        for dz in (-1, 0, 1)
        if (dx, dy, dz) != (0, 0, 0)
    ]

    def exists(d):
        flag = None
        for i in range(3):
            if d[i]:
                here = has[i][1 if d[i] > 0 else 0]
                flag = here if flag is None else jnp.logical_and(flag, here)
        return flag

    peers = {d: (exists(d), tuple(me[i] + d[i] for i in range(3))) for d in directions}
    far = [d for d in directions if d[1] and d[2]]
    far.sort(key=lambda d: abs(d[0]))
    up_down = [(0, 0, -1), (0, 0, 1)]
    cross = [d for d in directions if d[0] and d[2] and not d[1]]
    flat = [d for d in directions if not d[2]]
    flat.sort(key=lambda d: (-abs(d[1]), abs(d[0])))

    barrier = pltpu.get_barrier_semaphore()

    def greet(device, index):
        pl.semaphore_signal(barrier, inc=1, device_id=device, device_id_type=MESH)

    if max(counts) <= ROUNDS:
        for d in far[::-1] + cross + up_down + flat:

            @pl.when(peers[d][0])
            def _():
                greet(peers[d][1], 0)

        greeted = 1
        for i in range(3):
            low, high = has[i]
            greeted = greeted * (1 + low.astype(jnp.int32) + high.astype(jnp.int32))
        others = greeted - 1
    else:
        each_other(greet)
        others = counts[0] * counts[1] * counts[2] - 1

    for load in loads[2:]:
        load.start()

    sub8 = lax.broadcasted_iota(jnp.int32, (8, 128), 0)
    lane8 = lax.broadcasted_iota(jnp.int32, (8, 128), 1)
    ex, ey = (lane8 // 4) % 4, lane8 % 4
    low_x, high_x = lane8 < 16, lane8 >= 112
    join_low_x, join_high_x = low_x & (ex > 0), high_x & (ex < 3)
    join_low_y, join_high_y = (sub8 == 0) & (ey > 0), (sub8 == 7) & (ey < 3)
    pack_b = lane8 // 16
    pack_low_y, pack_high_y = (pack_b == 0) & (ey > 0), (pack_b == 7) & (ey < 3)
    origin = [(lane8 - 3 - (lane8 + 1) % 4) % 128, (lane8 + 3 - lane8 % 4) % 128]
    edge_join_low = [(o < 16) & ((o // 4) % 4 > 0) for o in origin]
    edge_join_high = [(o >= 112) & ((o // 4) % 4 < 3) for o in origin]
    far_y = ((sub8 == 0) & (ey == 0)) | ((sub8 == 7) & (ey == 3))
    far_low = (sub8 == 0) & ((lane8 == 0) | (lane8 == 124))
    far_high = (sub8 == 7) & ((lane8 == 3) | (lane8 == 127))
    far_corner = far_low | far_high
    edge_low_y, edge_high_y = (pack_b == 0) & (ey == 0), (pack_b == 7) & (ey == 3)

    def half(flag):
        return jnp.where(flag, 0.5, 1.0).astype(f32)

    total = [BX * counts[0], BY * counts[1], BZ * counts[2]]
    pos_x, pos_y = ex + me[0] * BX, ey + me[1] * BY
    share_xy = half((low_x & (pos_x > 0)) | (high_x & (pos_x < total[0] - 1)))
    share_xy = share_xy * half(
        ((sub8 == 0) & (pos_y > 0)) | ((sub8 == 7) & (pos_y < total[1] - 1))
    )
    share_xy = share_xy.reshape(1, 8, 128)
    share = [share_xy] * 8
    share[0] = share_xy * half(has[2][0])
    share[7] = share_xy * half(has[2][1])

    def turn(x, shift, axis):
        size = x.shape[axis]
        shift = shift % size
        return pltpu.roll(x, shift, axis) if shift else x

    def rows_of(ref, count):
        return [
            jnp.stack([ref[k, pl.ds(b, 8, stride=8), :] for k in range(count)])
            for b in range(8)
        ]

    def planes_of(ref, count):
        return [
            jnp.stack([ref[k, 8 * c : 8 * c + 8, :] for k in range(count)]) for c in range(8)
        ]

    def put_rows(ref, rows):
        for b in range(8):
            for k in range(rows[b].shape[0]):
                ref[k, pl.ds(b, 8, stride=8), :] = rows[b][k]

    def put_planes(ref, planes):
        for c in range(8):
            for k in range(planes[c].shape[0]):
                ref[k, 8 * c : 8 * c + 8, :] = planes[c][k]

    loads[0].wait()
    r16 = lax.broadcasted_iota(jnp.int32, (16, 16), 0)
    l16 = lax.broadcasted_iota(jnp.int32, (16, 16), 1)
    by_lane = jnp.zeros((16, 16), jnp.int32)
    by_row = jnp.zeros((16, 16), jnp.int32)
    for e in range(16):
        by_lane = jnp.where(l16 == e, place_ref[e], by_lane)
        by_row = jnp.where(r16 == e, place_ref[e], by_row)
    to_place = jnp.concatenate([(by_lane == r16).astype(f32)] * 3, axis=1)
    to_slot = jnp.concatenate([(by_row == l16).astype(f32)] * 3, axis=1)

    def order(matrix, block):
        high = block.astype(jnp.bfloat16).astype(f32)
        rest = block - high
        middle = rest.astype(jnp.bfloat16).astype(f32)
        parts = jnp.concatenate([high, middle, rest - middle], axis=0)
        return jnp.dot(
            matrix.astype(jnp.bfloat16),
            parts.astype(jnp.bfloat16),
            preferred_element_type=f32,
        )

    lane64 = lax.broadcasted_iota(jnp.int32, (64, 128), 1)

    def take(first, second):
        blocks = [
            order(to_place, field)[:, 128 * t : 128 * t + 128]
            for field in (first, second)
            for t in range(4)
        ]
        turned = jnp.concatenate(blocks, axis=0).T
        top, bottom = turned[:64], turned[64:]
        left = jnp.where(lane64 < 64, top, turn(bottom, 64, 1))
        right = jnp.where(lane64 < 64, turn(top, 64, 1), bottom)
        return left, right

    def give(first, second):
        for k, field in enumerate((first, second)):
            for c in range(8):
                work_d[k, 8 * c : 8 * c + 8, :] = field[c].reshape(8, 128)
        left, right = (
            jnp.concatenate(
                [work_d[k, pl.ds(b, 8, stride=8), :] for b in range(8)], axis=0
            )
            for k in range(2)
        )
        top = jnp.where(lane64 < 64, left, turn(right, 64, 1))
        bottom = jnp.where(lane64 < 64, turn(left, 64, 1), right)
        turned = jnp.concatenate([top, bottom], axis=0).T
        return [
            order(
                to_slot,
                jnp.concatenate(
                    [turned[64 * k + 16 * t : 64 * k + 16 * t + 16] for t in range(4)], axis=1
                ),
            )
            for k in range(2)
        ]

    loads[1].wait()
    loads[2].wait()
    taken = [*take(vel_ref[0], vel_ref[1]), *take(vel_ref[2], den_ref[...])]
    put_rows(
        work_v, [jnp.stack([f[8 * b : 8 * b + 8] for f in taken]) for b in range(8)]
    )
    planes = planes_of(work_v, 4)
    velocity = [planes[c][0:3] for c in range(8)]

    def split(x):
        high = x.astype(jnp.bfloat16)
        low = (x - high.astype(f32)).astype(jnp.bfloat16)
        return jnp.concatenate([high, low, high], axis=1)

    def along_y(v, matrix, sign):
        c = v[0].shape[0]
        put_planes(work_v, v)
        put_rows(work_d, along_index(matrix, sign, rows_of(work_v, c)))
        return planes_of(work_d, c)

    def code(d):
        return (d[0] + 1) * 9 + (d[1] + 1) * 3 + d[2] + 1

    def side_of(step):
        return 1 if step > 0 else 0

    def column(dx, dy):
        return 3 * (dx + 1) + dy + 1

    def edge_slot(d):
        if d[0] and d[1]:
            return 8 + 4 * side_of(d[0]) + 2 * side_of(d[1]) + side_of(d[2])
        return (0 if d[0] else 4) + 2 * side_of(d[0] or d[1]) + side_of(d[2])

    def source(r, d, c):
        if not d[0] and not d[1]:
            return send_z.at[r, side_of(d[2]), pl.ds(0, c)]
        if d[2]:
            return send_e.at[r, edge_slot(d)]
        return (send_x if d[0] else send_y).at[r, side_of(d[0] if d[0] else d[1])]

    def target(r, d, c):
        if not d[0] and not d[1]:
            return recv_z.at[r, side_of(d[2]), pl.ds(0, c)]
        if d[2]:
            return recv_e.at[r, code(d)]
        return recv_xy.at[r, column(d[0], d[1])]

    def copy(r, d, c, incoming):
        back = d if incoming else tuple(-i for i in d)
        return pltpu.make_async_remote_copy(
            src_ref=source(r, d, c),
            dst_ref=target(r, back, c),
            send_sem=send_sem.at[code(d)],
            recv_sem=recv_sem.at[r, code(back)],
            device_id=peers[d][1],
            device_id_type=MESH,
        )

    def start(r, c, group):
        for d in group:

            @pl.when(peers[d][0])
            def _():
                copy(r, d, c, False).start()

    def finish(r, c, group):
        for d in group[::-1]:

            @pl.when(peers[d][0])
            def _():
                copy(r, d, c, True).wait_recv()

    def sent():
        for d in directions:
            if not d[0] and not d[1]:
                ref = recv_z.at[pl.ds(0, 2)]
            elif d[2]:
                ref = recv_e.at[:, 0]
            else:
                ref = recv_xy.at[:, 0]

            @pl.when(peers[d][0])
            def _():
                pltpu.make_async_remote_copy(
                    src_ref=ref,
                    dst_ref=ref,
                    send_sem=send_sem.at[code(d)],
                    recv_sem=recv_sem.at[0, code(d)],
                    device_id=peers[d][1],
                    device_id_type=MESH,
                ).wait_send()

    def clear():
        for d in directions:

            @pl.when(jnp.logical_not(peers[d][0]))
            def _():
                for r in range(ROUNDS):
                    if not d[0] and not d[1]:
                        recv_z[r, side_of(d[2])] = jnp.zeros((4, 8, 128), f32)
                    elif d[2]:
                        recv_e[r, code(d)] = jnp.zeros((1, 128), f32)
                    else:
                        recv_xy[r, column(d[0], d[1])] = jnp.zeros((8, 128), f32)

    def join_x(v):
        low, high = turn(v, 20, 2), turn(v, -20, 2)
        return v + jnp.where(join_low_x, low, jnp.where(join_high_x, high, 0.0))

    def join_y(v):
        low, high = turn(turn(v, 1, 1), 1, 2), turn(turn(v, -1, 1), -1, 2)
        return v + jnp.where(join_low_y, low, jnp.where(join_high_y, high, 0.0))

    def join_xy(v):
        up, down = turn(v, 1, 1), turn(v, -1, 1)
        low, high = turn(v, 20, 2), turn(v, -20, 2)
        out = v + jnp.where(join_low_x, low, jnp.where(join_high_x, high, 0.0))
        for face, step, mask in ((up, 1, join_low_y), (down, -1, join_high_y)):
            part = turn(face, step, 2)
            low, high = turn(face, step + 20, 2), turn(face, step - 20, 2)
            part = part + jnp.where(join_low_x, low, jnp.where(join_high_x, high, 0.0))
            out = out + jnp.where(mask, part, 0.0)
        return out

    def merge(parts, index, bit=1):
        while len(parts) > 1:
            parts = [
                jnp.where((index & bit) == 0, parts[i], parts[i + 1])
                for i in range(0, len(parts), 2)
            ]
            bit *= 2
        return parts[0]

    def by_slot(parts, slot):
        acc = parts[0]
        for k in range(1, len(parts)):
            acc = jnp.where(slot == k, parts[k], acc)
        return acc

    def edge_rows(r, dx, dy):
        low, high = recv_e[r, code((dx, dy, -1))], recv_e[r, code((dx, dy, 1))]
        return jnp.where(sub8 == 0, low, jnp.where(sub8 == 7, high, 0.0))

    def send_far(r, dz, v):
        c = v.shape[0]
        for side, dy in enumerate((-1, 1)):
            shift = -3 * dy if side else 3
            slot = (ey + 1 - side) % 4
            face = by_slot([turn(v[k], k + shift, 1) for k in range(c)], slot)
            low = by_slot([turn(v[k], k + shift + 20, 1) for k in range(c)], slot)
            high = by_slot([turn(v[k], k + shift - 20, 1) for k in range(c)], slot)
            face = face + jnp.where(
                edge_join_low[side], low, jnp.where(edge_join_high[side], high, 0.0)
            )
            row = 7 * side
            send_e[r, edge_slot((0, dy, dz))] = face[row : row + 1]
            for dx in (-1, 1):
                shift_x = -124 * dx - 3 * dy
                corner = by_slot(
                    [turn(v[k], shift_x + 16 * k, 1) for k in range(c)],
                    ((lane8 + 4) // 16) % 8,
                )
                send_e[r, edge_slot((dx, dy, dz))] = corner[row : row + 1]

    def take_far(r, dz, c):
        face = jnp.where(
            sub8 == 0,
            recv_e[r, code((0, -1, dz))],
            jnp.where(sub8 == 7, recv_e[r, code((0, 1, dz))], 0.0),
        )
        inner = lane8 % 16 < 4
        rows = [
            jnp.where(inner, recv_e[r, code((-1, dy, dz))], recv_e[r, code((1, dy, dz))])
            for dy in (-1, 1)
        ]
        corner = jnp.where(sub8 == 0, rows[0], jnp.where(sub8 == 7, rows[1], 0.0))
        return jnp.stack(
            [
                jnp.where(far_y, turn(face, -k, 1), 0.0)
                + jnp.where(far_corner, turn(corner, -16 * k, 1), 0.0)
                for k in range(c)
            ]
        )

    def assemble(v, r, hook=None):
        for side in range(2):
            send_far(r, 2 * side - 1, v[7 * side])
        c = v[0].shape[0]
        for side in range(2):
            send_z[r, side, pl.ds(0, c)] = v[7 * side]
        v = list(v)
        put_planes(work_g, v)
        rows = [
            [work_g[k, pl.ds(b, 8, stride=8), :] for k in range(c)] for b in range(8)
        ]
        for side in range(2):
            own = rows[7 * side]
            face = by_slot([turn(own[k], k - 3 * side, 1) for k in range(c)], ey)
            low = by_slot([turn(own[k], k - 3 * side + 20, 1) for k in range(c)], ey)
            high = by_slot([turn(own[k], k - 3 * side - 20, 1) for k in range(c)], ey)
            send_y[r, side] = face + jnp.where(
                join_low_x, low, jnp.where(join_high_x, high, 0.0)
            )
        start(r, c, far + flat[:2] + up_down)
        for side in range(2):
            packed = []
            for b in range(8):
                shift = 16 * b - 124 * side
                packed.append(by_slot([turn(rows[b][k], shift + 4 * k, 1) for k in range(c)], ex))
            face = merge(packed, pack_b)
            shift = -124 * side
            low = by_slot([turn(rows[7][k], shift + 4 * k + 1, 1) for k in range(c)], ex)
            shift += 112
            high = by_slot([turn(rows[0][k], shift + 4 * k - 1, 1) for k in range(c)], ex)
            face = face + jnp.where(pack_low_y, low, jnp.where(pack_high_y, high, 0.0))
            send_x[r, side] = face
            send_e[r, 2 * side] = face[0:1]
            send_e[r, 2 * side + 1] = face[7:8]
        start(r, c, cross + flat[2:])
        for t in range(1, 7):
            v[t] = join_x(join_y(v[t]))
        if hook is not None:
            hook()
        finish(r, c, flat + up_down + cross)
        faces = [recv_xy[r, column(dx, 0)] + edge_rows(r, dx, 0) for dx in (-1, 1)]
        for side in range(2):
            v[7 * side] = join_xy(v[7 * side] + recv_z[r, side, :c])
        for b in range(8):
            for k in range(c):
                low = turn(faces[0], -16 * b - 4 * k, 1)
                high = turn(faces[1], 124 - 16 * b - 4 * k, 1)
                part = jnp.where(lane8 < 4, low, jnp.where(lane8 >= 124, high, 0.0))
                if b in (0, 7):
                    side = b // 7
                    dy, slot = 2 * side - 1, 3 * side
                    face = turn(recv_xy[r, column(0, dy)], slot - k, 1)
                    part = part + jnp.where(ey == slot, face, 0.0)
                    begin = slot - 4 * k - 115 * (1 - side)
                    low = turn(recv_xy[r, column(-1, dy)], begin, 1)
                    high = turn(recv_xy[r, column(1, dy)], begin + 124, 1)
                    part = part + jnp.where(
                        lane8 == slot, low, jnp.where(lane8 == 124 + slot, high, 0.0)
                    )
                work_c[k, pl.ds(b, 8, stride=8), :] = part
        corrections = planes_of(work_c, c)
        v = [v[t] + corrections[t] for t in range(8)]
        finish(r, c, far)
        for side in range(2):
            v[7 * side] = v[7 * side] + take_far(r, 2 * side - 1, c)
        return v

    def along_x(v, w_ref):
        c = v[0].shape[0]
        x = jnp.concatenate([v[t].reshape(c * 8, 128) for t in range(8)], axis=0)
        y = jnp.dot(split(x), w_ref[...], preferred_element_type=f32)
        return [y[t * c * 8 : (t + 1) * c * 8].reshape(c, 8, 128) for t in range(8)]

    def advect(v):
        dx = along_x(v, fwd_ref)
        dy = along_y(v, deriv, -1)
        dz = along_index(deriv, -1, v)
        return [
            velocity[t][0:1] * dx[t] + velocity[t][1:2] * dy[t] + velocity[t][2:3] * dz[t]
            for t in range(8)
        ]

    loads[3].wait()
    diag, quad, mobile = [], [], []

    def diagonal():
        clear()
        for load in loads[4:]:
            load.wait()
        plane = plane_ref[...].reshape(1, 8, 128)
        quad.extend(plane * float(weights[t]) for t in range(8))
        mobile.extend(quad[t] * planes[t][3:4] for t in range(8))
        square_x = along_x(mobile, sqr_ref)
        square_y = along_y(mobile, squared_t, 1)
        square_z = along_index(squared_t, 1, mobile)
        diag.extend(
            mass_shift * quad[t] + square_x[t] + square_y[t] + square_z[t] for t in range(8)
        )

    rate = advect(velocity)
    pl.semaphore_wait(barrier, others)
    total_rate = None
    for r, step, weight in ((0, 0.5, 1.0), (1, 0.5, 2.0), (2, 1.0, 2.0), (3, 0.0, 1.0)):
        if r == 1:
            rate = [jnp.concatenate([rate[t], diag[t]], axis=0) for t in range(8)]
        g = assemble(rate, r, None if r else diagonal)
        if r == 1:
            inverse_jacobi = [1.0 / g[t][3:4] for t in range(8)]
        g = [g[t][0:3] * share[t] for t in range(8)]
        total_rate = [weight * g[t] + (total_rate[t] if r else 0.0) for t in range(8)]
        if step:
            rate = advect([velocity[t] - (step * time_step) * g[t] for t in range(8)])
    advected = [velocity[t] - (time_step / 6.0) * total_rate[t] for t in range(8)]
    div_x = along_x([advected[t][0:1] for t in range(8)], fwd_ref)
    div_y = along_y([advected[t][1:2] for t in range(8)], deriv, -1)
    div_z = along_index(deriv, -1, [advected[t][2:3] for t in range(8)])
    div = [div_x[t] + div_y[t] + div_z[t] for t in range(8)]

    def put_advected():
        parts = [[advected[t][i] for t in range(8)] for i in range(3)]
        adv_ref[0], adv_ref[1] = give(parts[0], parts[1])
        adv_ref[2], _ = give(parts[2], parts[2])

    total_div = assemble(div, 4, put_advected)
    r0 = [total_div[t] * (quad[t] * (-1.0 / time_step)) for t in range(8)]

    def slopes(v):
        return along_x(v, fwd_ref), along_y(v, deriv, -1), along_index(deriv, -1, v)

    def flux(slope):
        return [[mobile[t] * part[t] for t in range(8)] for part in slope]

    def local(v, flow):
        bx = along_x(flow[0], bwd_ref)
        by = along_y(flow[1], deriv_t, -1)
        bz = along_index(deriv_t, -1, flow[2])
        return [(mass_shift * quad[t]) * v[t] + bx[t] + by[t] + bz[t] for t in range(8)]

    def energy_row(v, slope, flow):
        acc = None
        for t in range(8):
            term = (mass_shift * quad[t]) * (v[t] * v[t])
            for i in range(3):
                term = term + flow[i][t] * slope[i][t]
            acc = term if acc is None else acc + term
        return jnp.sum(acc[0], axis=0, keepdims=True)

    def dot_row(a, b, scale=None):
        acc = None
        for t in range(8):
            term = a[t] * b[t]
            if scale is not None:
                term = term * scale[t]
            acc = term if acc is None else acc + term
        return jnp.sum(acc[0], axis=0, keepdims=True)

    given = {}

    def give_first():
        given["r0"], given["z0"] = give(r0, z0)

    def give_second():
        given["s"], given["w"] = give(s, w)

    z0 = [r0[t] * inverse_jacobi[t] for t in range(8)]
    slope = slopes(z0)
    flow = flux(slope)
    rho_row = dot_row(r0, z0, share)
    gamma_row = energy_row(z0, slope, flow)

    s = assemble(local(z0, flow), 5, give_first)
    w = [s[t] * inverse_jacobi[t] for t in range(8)]
    delta_row = dot_row(s, w, share)
    slope = slopes(w)
    flow = flux(slope)
    eps_row = energy_row(w, slope, flow)
    partial = jnp.concatenate(
        [rho_row, gamma_row, delta_row, eps_row, jnp.zeros((4, 128), f32)], axis=0
    )
    partial = jnp.sum(partial, axis=1, keepdims=True)
    own = jnp.sum(jnp.where(sub8 == lane8, partial, 0.0), axis=0, keepdims=True)
    sums[...] = own

    def share_sums(device, index):
        pltpu.make_async_remote_copy(
            src_ref=sums,
            dst_ref=sums_in.at[index],
            send_sem=sum_send,
            recv_sem=sum_recv,
            device_id=device,
            device_id_type=MESH,
        ).start()

    each_other(share_sums)
    t_vec = assemble(local(w, flow), 6, give_second)
    third, _ = give(t_vec, t_vec)
    arrived = pltpu.make_async_remote_copy(
        src_ref=sums_in,
        dst_ref=sums_in,
        send_sem=sum_send,
        recv_sem=sum_recv,
        device_id=tuple(lax.rem(me[i] + 1, counts[i]) for i in range(3)),
        device_id_type=MESH,
    )
    sent()
    arrived.wait_send()
    arrived.wait_recv()
    joined = own + jnp.sum(sums_in[...], axis=0)
    four = jnp.sum(jnp.where(sub8 == lane8, joined, 0.0), axis=1, keepdims=True)
    rho, gamma, delta, eps = (four[i : i + 1] for i in range(4))
    alpha0 = rho / gamma
    rho1 = rho - 2.0 * alpha0 * gamma + alpha0 * alpha0 * delta
    beta = rho1 / rho
    cross = gamma - alpha0 * delta
    curve = gamma - 2.0 * alpha0 * delta + alpha0 * alpha0 * eps
    curve = curve + 2.0 * beta * cross + beta * beta * gamma
    alpha1 = rho1 / curve
    along = alpha0 + alpha1 * (1.0 + beta)
    side_step = alpha0 * alpha1

    pre_ref[...] = along * given["z0"] - side_step * given["w"]
    res_ref[...] = given["r0"] - along * given["s"] + side_step * third


def finish_kernel(adv_ref, pre_ref, res_ref, adv_out, pre_out, res_out):
    adv_out[...] = adv_ref[...]
    pre_out[...] = pre_ref[...]
    res_out[...] = res_ref[...]


def per_device(counts, velocity, inv_density, element_place):
    f32 = jnp.float32
    plane, forward, backward, square = constants()
    elements = element_place.shape[0]
    points = inv_density.shape[0]
    vmem = pl.BlockSpec(memory_space=pltpu.VMEM)
    faces = pltpu.VMEM((ROUNDS, 2, 8, 128), f32)
    faces_z = pltpu.VMEM((ROUNDS, 2, 4, 8, 128), f32)
    work = pltpu.VMEM((4, 64, 128), f32)
    dma = pltpu.SemaphoreType.DMA
    others = counts[0] * counts[1] * counts[2] - 1
    shapes = (
        jax.ShapeDtypeStruct((3, elements, points), f32),
        jax.ShapeDtypeStruct((elements, points), f32),
        jax.ShapeDtypeStruct((elements, points), f32),
    )
    computed = pl.pallas_call(
        functools.partial(kernel, counts),
        out_shape=shapes,
        in_specs=[pl.BlockSpec(memory_space=pltpu.HBM)] * 7,
        out_specs=(vmem, vmem, vmem),
        scratch_shapes=[
            faces,
            faces,
            faces_z,
            pltpu.VMEM((ROUNDS, 16, 1, 128), f32),
            pltpu.VMEM((ROUNDS, 9, 8, 128), f32),
            faces_z,
            pltpu.VMEM((ROUNDS, 27, 1, 128), f32),
            work,
            work,
            work,
            work,
            pltpu.VMEM((1, 128), f32),
            pltpu.VMEM((others, 1, 128), f32),
            dma((27,)),
            dma((ROUNDS, 27)),
            dma,
            dma,
            pltpu.VMEM((3, elements, points), f32),
            pltpu.VMEM((elements, points), f32),
            pltpu.SMEM((elements,), jnp.int32),
            pltpu.VMEM(plane.shape, f32),
            pltpu.VMEM(forward.shape, jnp.bfloat16),
            pltpu.VMEM(backward.shape, jnp.bfloat16),
            pltpu.VMEM(square.shape, jnp.bfloat16),
            dma((7,)),
        ],
        compiler_params=pltpu.CompilerParams(
            collective_id=0, has_side_effects=True, vmem_limit_bytes=VMEM_LIMIT
        ),
    )(
        *(
            pltpu.with_memory_space_constraint(operand, pltpu.HBM)
            for operand in (
                velocity.transpose(0, 2, 1),
                inv_density.T,
                element_place,
                jnp.asarray(plane),
                jnp.asarray(forward),
                jnp.asarray(backward),
                jnp.asarray(square),
            )
        )
    )
    advected, pressure, residual = pl.pallas_call(
        finish_kernel,
        out_shape=shapes,
        in_specs=[vmem, vmem, vmem],
        out_specs=(vmem, vmem, vmem),
        compiler_params=pltpu.CompilerParams(vmem_limit_bytes=VMEM_LIMIT),
    )(*computed)
    return advected.transpose(0, 2, 1), pressure.T, residual.T


def solution(mesh):
    counts = tuple(mesh.shape[name] for name in AXES)
    placed = (P(None, None, AXES), P(None, AXES), P(AXES))
    return jax.shard_map(
        functools.partial(per_device, counts),
        mesh=mesh,
        in_specs=placed,
        out_specs=(P(None, None, AXES), P(None, AXES), P(None, AXES)),
        check_vma=False,
    )
```
